32 devices in a mesh: groups: 2 (over x), seq: 4 (over y, core), head: 4 (over z).
Axes of the slice: x: 2, y: 2, z: 4, core: 2. Of those that a mesh axis runs over, the one named last changes fastest.
Arguments:
- queries: bfloat16 [1024, 8192], P(('groups', 'seq'), 'head'), parts along dimension 0
- new_keys: bfloat16 [1024, 1024], P(('groups', 'seq'), 'head'), parts along dimension 0, may hold values from -6 to 6
- new_values: bfloat16 [1024, 1024], P(('groups', 'seq'), 'head'), parts along dimension 0, may hold values from -6 to 6
- cache_keys: bfloat16 [8192, 1024], P(('groups', 'seq'), 'head'), parts along dimension 0
- cache_values: bfloat16 [8192, 1024], P(('groups', 'seq'), 'head'), parts along dimension 0, may hold values from -6 to 6
- valid_len: int32 [8], P('groups'), parts along dimension 0, may hold values from 1 to 1024, as said below
- block_of: int32 [8], P('groups'), parts along dimension 0, may hold values from 0 to 3, each once
Outputs:
- attended: bfloat16 [1024, 8192], P(('groups', 'seq'), 'head'), parts along dimension 0
The draws below stay inside these ranges and needn't reach their ends.
There are 2 independent parts, one for each index of `groups`. The reference program is written for one: setup_inputs(seed, part) draws one part's arguments, and reference() takes and returns one part's arrays. A program takes and returns all parts, laid end to end along the dimension named above; each array names one. Nothing has to cross between parts.
Inputs may be any that keep to these rules, and one draw needn't show every extreme that they name: `valid_len`: some shard is full (1024 filled slots) in every draw; slot 0 of every shard is filled. `block_of`: A permutation of the 4 span blocks.
All inputs are finite; a program needn't handle non-finite values.
Results may differ from the reference program's by a relative error of at most 0.0027.
Values may be sent and summed in bfloat16 or wider, within the bound.
A program may use at most 192 MiB of HBM per device.

```python
import math
import jax
import jax.numpy as jnp
from jax import lax

HQ = 64
KV = 8
DH = 128
GROUP = 8
CB = 128
LEN_DEV = 1024
SPAN = 512
CONTEXT = 4096
N_SEQ = 4


def draw_queries(key, part):
    shape = (SPAN, HQ * DH)
    drawn = jnp.clip(jax.random.normal(key, shape, jnp.float32), -6.0, 6.0)
    return drawn.astype(jnp.bfloat16)


def draw_cache_keys(key, part):
    shape = (CONTEXT, KV * DH)
    drawn = jnp.clip(jax.random.normal(key, shape, jnp.float32), -6.0, 6.0)
    return drawn.astype(jnp.bfloat16)


def draw_valid_len(key, part):
    filled = jax.random.randint(jax.random.fold_in(key, 3), (N_SEQ,), 1, LEN_DEV + 1)
    full_one = jax.random.randint(jax.random.fold_in(key, 5), (), 0, N_SEQ)
    return filled.at[full_one].set(LEN_DEV).astype(jnp.int32)


def shard_levels(rng, shape, cuts, smallest, largest):
    factor_of, own = 1.0, jax.random.fold_in(rng, 6)
    for axis_at, parts in cuts:
        heights = jnp.exp(jax.random.uniform(jax.random.fold_in(own, axis_at), (parts,), jnp.float32, smallest / len(cuts), largest / len(cuts)))
        factor_of = factor_of * jnp.repeat(heights, shape[axis_at] // parts).reshape([-1 if axis == axis_at else 1 for axis in range(len(shape))])
    return factor_of


def bell_draw(key, dims, scale, limit, pieces=(), kind=jnp.bfloat16):
    values = scale * jax.random.normal(key, dims, jnp.float32)
    if pieces:
        values = values * shard_levels(key, dims, pieces, -0.22, 0.18)
    return jnp.clip(values, -limit, limit).astype(kind)


def setup_inputs(seed: int = 0, part: int = 0) -> dict:
    streams_of = jax.random.split(jax.random.key(seed), 8)
    part_splits = jax.random.split(jax.random.fold_in(streams_of[7], part), 8)
    queries = draw_queries(jax.random.fold_in(jax.random.fold_in(streams_of[7], part), 71), part)
    new_keys = bell_draw(part_splits[1], (SPAN, KV * DH), 1.0, 6.0, ((0, 4), (1, 4)))
    new_values = bell_draw(part_splits[2], (SPAN, KV * DH), 1.0, 6.0, ((0, 4), (1, 4)))
    cache_keys = draw_cache_keys(jax.random.fold_in(jax.random.fold_in(streams_of[7], part), 71), part)
    cache_values = bell_draw(part_splits[4], (CONTEXT, KV * DH), 1.0, 6.0, ((0, 4), (1, 4)))
    valid_len = draw_valid_len(jax.random.fold_in(jax.random.fold_in(streams_of[7], part), 71), part)
    block_of = jax.random.permutation(part_splits[6], N_SEQ).astype(jnp.int32)
    return dict(queries=queries, new_keys=new_keys, new_values=new_values, cache_keys=cache_keys, cache_values=cache_values, valid_len=valid_len, block_of=block_of)


def reference(queries, new_keys, new_values, cache_keys, cache_values, valid_len, block_of):
    span = CB * N_SEQ
    context = LEN_DEV * N_SEQ
    rows = jnp.arange(span, dtype=jnp.int32)
    query_pos = block_of[rows // CB].astype(jnp.int32) * CB + rows % CB
    places = jnp.arange(context, dtype=jnp.int32)
    cache_live = (places % LEN_DEV) < valid_len[places // LEN_DEV]
    key_pos = jnp.concatenate([jnp.full((context,), -1, jnp.int32), query_pos])
    key_live = jnp.concatenate([cache_live, jnp.ones((span,), bool)])
    keys_all = jnp.concatenate([cache_keys, new_keys], 0).astype(jnp.float32).reshape(-1, KV, DH)
    values_cache = cache_values.astype(jnp.float32).reshape(N_SEQ, LEN_DEV, KV, DH)
    values_span = new_values.astype(jnp.float32).reshape(N_SEQ, CB, KV, DH)
    width = math.gcd(span, 16)
    count = span // width
    query_blocks = queries.astype(jnp.float32).reshape(count, width, KV, GROUP, DH)
    pos_blocks = query_pos.reshape(count, width)

    def one_block(item):
        block, pos = item
        scores = jnp.einsum("rkgd,nkd->rkgn", block, keys_all) * (DH ** -0.5)
        seen = (key_live[None, :] & (key_pos[None, :] <= pos[:, None]))[:, None, None, :]
        masked = jnp.where(seen, scores, -1.0e30)
        lead = masked.shape[:3]
        cache_part = masked[..., :context].reshape(lead + (N_SEQ, LEN_DEV))
        span_part = masked[..., context:].reshape(lead + (N_SEQ, CB))
        local = jnp.maximum(jnp.max(cache_part, axis=-1), jnp.max(span_part, axis=-1))
        local_full = jnp.concatenate([jnp.repeat(local, LEN_DEV, axis=-1), jnp.repeat(local, CB, axis=-1)], -1)
        weights = jnp.where(seen, jnp.exp(scores - local_full), 0.0)
        rounded = lax.optimization_barrier(weights.astype(jnp.bfloat16)).astype(jnp.float32)
        weights_cache = weights[..., :context].reshape(lead + (N_SEQ, LEN_DEV))
        weights_span = weights[..., context:].reshape(lead + (N_SEQ, CB))
        part_total = jnp.sum(weights_cache, axis=-1) + jnp.sum(weights_span, axis=-1)
        rounded_cache = rounded[..., :context].reshape(lead + (N_SEQ, LEN_DEV))
        rounded_span = rounded[..., context:].reshape(lead + (N_SEQ, CB))
        part_numer = jnp.einsum("rkgsl,slkd->rkgsd", rounded_cache, values_cache)
        part_numer = part_numer + jnp.einsum("rkgsc,sckd->rkgsd", rounded_span, values_span)
        top = jnp.max(local, axis=-1)
        factor = jnp.exp(local - top[..., None])
        numer = jnp.sum(part_numer * factor[..., None], axis=-2)
        total = jnp.sum(part_total * factor, axis=-1)
        return (numer / total[..., None]).astype(jnp.bfloat16).reshape(width, -1)

    result = lax.map(one_block, (query_blocks, pos_blocks))
    return result.reshape(span, HQ * DH)
```

```python
import functools
import math

import jax
import jax.numpy as jnp
from jax import lax
from jax.experimental import pallas as pl
from jax.experimental.pallas import tpu as pltpu
from jax.sharding import PartitionSpec as P

DH = 128
GROUP = 8
NEGATIVE = -1e30
TO_LOG2 = DH ** (-0.5) * math.log2(math.e)
CODE_MAX = 32767.0
UNROLL = 2


def kernel(
    n, pair, chunk,
    q_hbm, nk_hbm, nv_hbm, ck_hbm, cv_hbm, valid_hbm, block_hbm,
    out_ref,
    kbuf, vbuf, qbuf, numer, stats, code_out, code_in, stat_out, stat_in,
    cache_bias, span_bias, pad, valid_ref, block_ref,
    loc_sem, kv_send, kv_recv, q_send, q_recv, r_send, r_recv, s_send, s_recv,
):
    chips = n // pair
    rows, cols = q_hbm.shape
    length = ck_hbm.shape[0]
    per = length + rows
    heads = cols // DH
    chunks = heads // chunk
    width = chunk * DH
    me = lax.axis_index("seq")
    chip, core = me // pair, me % pair
    partner = chip * pair + (pair - 1 - core)

    def ahead(d):
        return ((chip + d) % chips) * pair + core

    def behind(d):
        return ((chip + chips - d) % chips) * pair + core

    sources = (ck_hbm, nk_hbm, cv_hbm, nv_hbm)
    spans = ((0, length), (length, rows))

    def place(i, slot):
        buf = kbuf if i < 2 else vbuf
        start, size = spans[i % 2]
        return buf.at[pl.ds(slot * per + start, size), :]

    local = [
        pltpu.make_async_copy(sources[i], place(i, 0), loc_sem.at[i]) for i in range(4)
    ] + [
        pltpu.make_async_copy(q_hbm, qbuf.at[0], loc_sem.at[4]),
        pltpu.make_async_copy(valid_hbm, valid_ref, loc_sem.at[5]),
        pltpu.make_async_copy(block_hbm, block_ref, loc_sem.at[6]),
    ]
    for copy in local:
        copy.start()

    barrier = pltpu.get_barrier_semaphore()
    others = [ahead(d) for d in range(1, chips)] + ([partner] if pair > 1 else [])
    for other in others:
        pl.semaphore_signal(barrier, inc=1, device_id={"seq": other})
    pl.semaphore_wait(barrier, len(others))

    def columns(c):
        return pl.ds(c * width, width)

    def send_query(d, c):
        return pltpu.make_async_remote_copy(
            src_ref=q_hbm.at[:, columns(c)],
            dst_ref=qbuf.at[d, :, columns(c)],
            send_sem=q_send.at[d, c], recv_sem=q_recv.at[d, c],
            device_id={"seq": ahead(d)},
        )

    def send_codes(d, c):
        return pltpu.make_async_remote_copy(
            src_ref=code_out.at[d, :, columns(c)],
            dst_ref=code_in.at[d, :, columns(c)],
            send_sem=r_send.at[d, c], recv_sem=r_recv.at[d, c],
            device_id={"seq": behind(d)},
        )

    def send_stats(d, c):
        return pltpu.make_async_remote_copy(
            src_ref=stat_out.at[d, c], dst_ref=stat_in.at[d, c],
            send_sem=s_send.at[d, c], recv_sem=s_recv.at[d, c],
            device_id={"seq": behind(d)},
        )

    query_copies = {(d, c): send_query(d, c) for c in range(chunks) for d in range(1, chips)}
    kv_copies = []
    if pair > 1:
        kv_copies = [
            pltpu.make_async_remote_copy(
                src_ref=sources[i], dst_ref=place(i, 1),
                send_sem=kv_send.at[i], recv_sem=kv_recv.at[i],
                device_id={"seq": partner},
            )
            for i in range(4)
        ]
    for (d, c), copy in query_copies.items():
        if c == 0:
            copy.start()
    for copy in kv_copies:
        copy.start()
    for (d, c), copy in query_copies.items():
        if c > 0:
            copy.start()

    local[5].wait()
    local[6].wait()
    key_owner = [me, partner][:pair]
    slot_at = lax.broadcasted_iota(jnp.int32, (8, length), 1)
    for slot in range(pair):
        live = slot_at < valid_ref[key_owner[slot]]
        cache_bias[slot] = jnp.where(live, 0.0, NEGATIVE)
    row_at = lax.broadcasted_iota(jnp.int32, (rows, rows), 0)
    col_at = lax.broadcasted_iota(jnp.int32, (rows, rows), 1)
    for d in range(chips):
        row_pos = block_ref[behind(d)] * rows + row_at
        for slot in range(pair):
            seen = block_ref[key_owner[slot]] * rows + col_at <= row_pos
            span_bias[d, slot] = jnp.where(seen, 0.0, NEGATIVE)

    lane = lax.broadcasted_iota(jnp.int32, (rows, DH), 1)
    pad[...] = jnp.zeros_like(pad)

    def head_terms(d, c, h):
        at = pl.ds(pl.multiple_of((c * chunk + h) * DH, DH), DH)
        head = (c * chunk) // GROUP
        kv_at = pl.ds(head * DH, DH)
        scores = lax.dot_general(
            qbuf[d, :, at], kbuf[:, kv_at], (((1,), (1,)), ((), ())),
            preferred_element_type=jnp.float32,
        )
        pieces = []
        for slot in range(pair):
            base = slot * per
            pieces.append(
                scores[:, base : base + length] * TO_LOG2 + cache_bias[slot, 0:1, :]
            )
            pieces.append(
                scores[:, base + length : base + per] * TO_LOG2 + span_bias[d, slot]
            )
        logits = jnp.concatenate(pieces, axis=1)
        top = jnp.max(logits, axis=1, keepdims=True)
        weights = jnp.exp2(logits - top)
        total = jnp.sum(weights, axis=1, keepdims=True)
        value = jnp.dot(
            weights.astype(jnp.bfloat16), vbuf[:, kv_at], preferred_element_type=jnp.float32
        )
        return at, top, total, value

    def own_chunk(c):
        def body(step, carry):
            for u in range(UNROLL):
                h = step * UNROLL + u
                at, top, total, value = head_terms(0, c, h)
                numer[:, at] = value
                stats[c, 0] = jnp.where(lane == h, top, stats[c, 0])
                stats[c, 1] = jnp.where(lane == h, total, stats[c, 1])
            return carry

        stats[c] = jnp.ones_like(stats[c])
        lax.fori_loop(0, chunk // UNROLL, body, 0)

    def other_chunk(d, c):
        def body(step, carry):
            for u in range(UNROLL):
                h = step * UNROLL + u
                at, top, total, value = head_terms(d, c, h)
                size = jnp.maximum(jnp.max(jnp.abs(value), axis=1, keepdims=True), 1e-30)
                code_out[d, :, at] = (
                    jnp.round(value * (CODE_MAX / size)).astype(jnp.int32).astype(jnp.int16)
                )
                pad[0] = jnp.where(lane == h, top, pad[0])
                pad[1] = jnp.where(lane == h, total, pad[1])
                pad[2] = jnp.where(lane == h, size * (1.0 / CODE_MAX), pad[2])
            return carry

        lax.fori_loop(0, chunk // UNROLL, body, 0)
        for k in range(3):
            stat_out[d, c, k] = jnp.transpose(pad[k])[0:8]
        send_codes(d, c).start()
        send_stats(d, c).start()

    for i in (0, 1, 4, 2, 3):
        local[i].wait()
    for copy in kv_copies:
        copy.wait()
    early = chunks // 2
    for c in range(early):
        own_chunk(c)
    for c in range(chunks):
        for d in range(1, chips):
            query_copies[d, c].wait_recv()
            other_chunk(d, c)
    for c in range(early, chunks):
        own_chunk(c)

    for c in range(chunks):
        mine_top, mine_total = stats[c, 0], stats[c, 1]
        got = []
        for d in range(1, chips):
            send_codes(d, c).wait_recv()
            send_stats(d, c).wait_recv()
            three = []
            for k in range(3):
                pad[k, 0:8] = stat_in[d, c, k]
                three.append(jnp.transpose(pad[k]))
            got.append(three)
        top = mine_top
        for three in got:
            top = jnp.maximum(top, three[0])
        own_factor = jnp.exp2(mine_top - top)
        total = own_factor * mine_total
        factors = [jnp.exp2(three[0] - top) for three in got]
        for factor, three in zip(factors, got):
            total = total + factor * three[1]
        inverse = 1.0 / total
        own_factor = own_factor * inverse
        factors = [factor * three[2] * inverse for factor, three in zip(factors, got)]
        for h in range(chunk):
            at = pl.ds((c * chunk + h) * DH, DH)
            result = numer[:, at] * own_factor[:, h : h + 1]
            for d in range(1, chips):
                codes = code_in[d, :, at].astype(jnp.int32).astype(jnp.float32)
                result = result + codes * factors[d - 1][:, h : h + 1]
            out_ref[:, at] = result.astype(jnp.bfloat16)

    for c in range(chunks):
        for d in range(1, chips):
            query_copies[d, c].wait_send()
            send_codes(d, c).wait_send()
            send_stats(d, c).wait_send()


def on_device(queries, new_keys, new_values, cache_keys, cache_values, valid_len, block_of):
    n = lax.axis_size("seq")
    pair = 2 if n % 2 == 0 else 1
    chips = n // pair
    rows, cols = queries.shape
    kv_cols = new_keys.shape[1]
    length = cache_keys.shape[0]
    heads = cols // DH
    chunk = 4
    chunks = heads // chunk
    pinned = [
        pltpu.with_memory_space_constraint(x, pltpu.HBM)
        for x in (
            queries, new_keys, new_values, cache_keys, cache_values, valid_len, block_of,
        )
    ]
    everywhere = pl.BlockSpec(memory_space=pl.ANY)
    dma = pltpu.SemaphoreType.DMA
    keys = pair * (length + rows)
    return pl.pallas_call(
        functools.partial(kernel, n, pair, chunk),
        out_shape=pltpu.VMEM((rows, cols), jnp.bfloat16),
        in_specs=[everywhere] * 7,
        out_specs=pl.BlockSpec(memory_space=pltpu.VMEM),
        scratch_shapes=[
            pltpu.VMEM((keys, kv_cols), jnp.bfloat16),
            pltpu.VMEM((keys, kv_cols), jnp.bfloat16),
            pltpu.VMEM((chips, rows, cols), jnp.bfloat16),
            pltpu.VMEM((rows, cols), jnp.float32),
            pltpu.VMEM((chunks, 2, rows, DH), jnp.float32),
            pltpu.VMEM((chips, rows, cols), jnp.int16),
            pltpu.VMEM((chips, rows, cols), jnp.int16),
            pltpu.VMEM((chips, chunks, 3, 8, rows), jnp.float32),
            pltpu.VMEM((chips, chunks, 3, 8, rows), jnp.float32),
            pltpu.VMEM((pair, 8, length), jnp.float32),
            pltpu.VMEM((chips, pair, rows, rows), jnp.float32),
            pltpu.VMEM((3, rows, DH), jnp.float32),
            pltpu.SMEM(valid_len.shape, jnp.int32),
            pltpu.SMEM(block_of.shape, jnp.int32),
            dma((7,)), dma((4,)), dma((4,)),
            dma((chips, chunks)), dma((chips, chunks)),
            dma((chips, chunks)), dma((chips, chunks)),
            dma((chips, chunks)), dma((chips, chunks)),
        ],
        compiler_params=pltpu.CompilerParams(collective_id=0, has_side_effects=True, vmem_limit_bytes=28 * 1024 * 1024),
    )(*pinned)


def solution(mesh):
    placed = (
        P(("groups", "seq"), "head"),
        P(("groups", "seq"), "head"),
        P(("groups", "seq"), "head"),
        P(("groups", "seq"), "head"),
        P(("groups", "seq"), "head"),
        P("groups"),
        P("groups"),
    )
    return jax.shard_map(
        on_device,
        mesh=mesh,
        in_specs=placed,
        out_specs=P(("groups", "seq"), "head"),
        check_vma=False,
    )
```

```python
import functools
import math

import jax
import jax.numpy as jnp
from jax import lax
from jax.experimental import pallas as pl
from jax.experimental.pallas import tpu as pltpu
from jax.sharding import PartitionSpec as P

DH = 128
GROUP = 8
NEGATIVE = -1e30
TO_LOG2 = DH ** (-0.5) * math.log2(math.e)
CODE_MAX = 32767.0
STACK = 2
TILE = 256


def kernel(
    n, pair,
    q_hbm, nk_hbm, nv_hbm, ck_hbm, cv_hbm, valid_hbm, block_hbm,
    out_ref,
    kbuf, vraw, vbuf, qbuf, score_a, score_b, top_a, top_b, own, own_stat,
    code_out, code_in, stat_out, stat_in, span_bias, pad, valid_ref, block_ref,
    loc_sem, kv_send, kv_recv, q_send, q_recv, r_send, r_recv, s_send, s_recv,
):
    chips = n // pair
    rows, cols = q_hbm.shape
    length, kv_cols = ck_hbm.shape
    kv_heads = kv_cols // DH
    heads = cols // DH
    steps = heads // STACK
    width = STACK * DH
    cached = pair * length
    keys = cached + pair * rows
    tiles = [(t, min(TILE, cached - t)) for t in range(0, cached, TILE)]
    tiles += [(cached + t, min(TILE, keys - cached - t)) for t in range(0, keys - cached, TILE)]
    me = lax.axis_index("seq")
    chip, core = me // pair, me % pair
    partner = chip * pair + (pair - 1 - core)

    def ahead(d):
        return ((chip + d) % chips) * pair + (pair - 1 - core)

    def behind(d):
        return ((chip + chips - d) % chips) * pair + (pair - 1 - core)

    sources = (ck_hbm, nk_hbm, cv_hbm, nv_hbm)

    def place(i, slot):
        buf = kbuf if i < 2 else vraw
        start, size = ((slot * length, length), (cached + slot * rows, rows))[i % 2]
        return buf.at[pl.ds(start, size), :]

    local = [
        pltpu.make_async_copy(sources[i], place(i, 0), loc_sem.at[i]) for i in range(4)
    ] + [
        pltpu.make_async_copy(q_hbm, qbuf.at[0], loc_sem.at[4]),
        pltpu.make_async_copy(valid_hbm, valid_ref, loc_sem.at[5]),
        pltpu.make_async_copy(block_hbm, block_ref, loc_sem.at[6]),
    ]
    for i in (4, 5, 6, 0, 1, 2, 3):
        local[i].start()

    barrier = pltpu.get_barrier_semaphore()
    others = [ahead(d) for d in range(1, chips)] + ([partner] if pair > 1 else [])
    for other in others:
        pl.semaphore_signal(barrier, inc=1, device_id={"seq": other})
    pl.semaphore_wait(barrier, len(others))

    def columns(p):
        return pl.ds(pl.multiple_of(p * width, width), width)

    def send_query(d, p):
        return pltpu.make_async_remote_copy(
            src_ref=qbuf.at[0, :, columns(p)],
            dst_ref=qbuf.at[d, :, columns(p)],
            send_sem=q_send.at[d, p], recv_sem=q_recv.at[d, p],
            device_id={"seq": ahead(d)},
        )

    def send_codes(d, p):
        return pltpu.make_async_remote_copy(
            src_ref=code_out.at[d, :, columns(p)],
            dst_ref=code_in.at[d, :, columns(p)],
            send_sem=r_send.at[d, p], recv_sem=r_recv.at[d, p],
            device_id={"seq": behind(d)},
        )

    def send_stats(d, p):
        return pltpu.make_async_remote_copy(
            src_ref=stat_out.at[d, p], dst_ref=stat_in.at[d, p],
            send_sem=s_send.at[d, p], recv_sem=s_recv.at[d, p],
            device_id={"seq": behind(d)},
        )

    kv_copies = []
    if pair > 1:
        kv_copies = [
            pltpu.make_async_remote_copy(
                src_ref=sources[i], dst_ref=place(i, 1),
                send_sem=kv_send.at[i], recv_sem=kv_recv.at[i],
                device_id={"seq": partner},
            )
            for i in range(4)
        ]
    local[4].wait()
    for d in range(1, chips):
        send_query(d, 0).start()
    for copy in kv_copies:
        copy.start()
    for p in range(1, steps):
        for d in range(1, chips):
            send_query(d, p).start()

    local[5].wait()
    local[6].wait()
    key_owner = [me, partner][:pair]
    row_at = lax.broadcasted_iota(jnp.int32, (rows, rows), 0)
    col_at = lax.broadcasted_iota(jnp.int32, (rows, rows), 1)
    for d in range(chips):
        row_pos = block_ref[behind(d) if d else me] * rows + row_at
        for slot in range(pair):
            seen = block_ref[key_owner[slot]] * rows + col_at <= row_pos
            span_bias[d, :, slot * rows : (slot + 1) * rows] = jnp.where(seen, 0.0, NEGATIVE)

    lane = lax.broadcasted_iota(jnp.int32, (rows, DH), 1)
    slot_at = lax.broadcasted_iota(jnp.int32, (TILE, DH), 0)
    ones = jnp.ones((TILE, DH), jnp.bfloat16)

    def live_rows(slot, t):
        live = slot_at + t < valid_ref[key_owner[slot]]
        return jnp.where(live, 1.0, 0.0).astype(jnp.bfloat16)

    def prepare_keys(slot):
        first = kbuf[slot * length : slot * length + 1, :]
        for t in range(0, length, TILE):
            at = pl.ds(slot * length + t, TILE)
            live = live_rows(slot, t)
            for h in range(kv_heads):
                part = pl.ds(h * DH, DH)
                kbuf[at, part] = kbuf[at, part] * live + first[:, h * DH : (h + 1) * DH] * (ones - live)

    def prepare_values(slot):
        for t in range(0, length, TILE):
            at = pl.ds(slot * length + t, TILE)
            live = live_rows(slot, t)
            for h in range(kv_heads):
                vbuf[at, 2 * h * DH : (2 * h + 1) * DH] = vraw[at, h * DH : (h + 1) * DH] * live
                vbuf[at, (2 * h + 1) * DH : (2 * h + 2) * DH] = live
        at = pl.ds(cached + slot * rows, rows)
        for h in range(kv_heads):
            vbuf[at, 2 * h * DH : (2 * h + 1) * DH] = vraw[at, h * DH : (h + 1) * DH]
            vbuf[at, (2 * h + 1) * DH : (2 * h + 2) * DH] = jnp.ones((rows, DH), jnp.bfloat16)

    score = (score_a, score_b)
    peak = (top_a, top_b)

    def find_scores(d, p, buf):
        query = qbuf[d, :, columns(p)]
        stacked = jnp.concatenate([query[:, u * DH : (u + 1) * DH] for u in range(STACK)], axis=0)
        kv_at = pl.ds(pl.multiple_of(p * STACK // GROUP * DH, DH), DH)
        best = None
        for start, size in tiles:
            part = lax.dot_general(
                stacked, kbuf[start : start + size, kv_at], (((1,), (1,)), ((), ())),
                preferred_element_type=jnp.float32,
            )
            if start >= cached:
                bias = span_bias[d, :, start - cached : start - cached + size]
                part = part + jnp.concatenate([bias] * STACK, axis=0)
            score[buf][:, start : start + size] = part
            for c in range(0, size, DH):
                piece = part[:, c : c + DH]
                best = piece if best is None else jnp.maximum(best, piece)
        peak[buf][...] = jnp.broadcast_to(jnp.max(best, axis=1, keepdims=True), peak[buf].shape)

    def attend(p, buf):
        kv_at = pl.ds(pl.multiple_of(p * STACK // GROUP * (2 * DH), 2 * DH), 2 * DH)
        top = peak[buf][...]
        both = None
        for start, size in tiles:
            weights = [
                jnp.exp2((score[buf][:, start + c : start + c + DH] - top) * TO_LOG2).astype(jnp.bfloat16)
                for c in range(0, size, DH)
            ]
            part = jnp.dot(
                jnp.concatenate(weights, axis=1), vbuf[start : start + size, kv_at],
                preferred_element_type=jnp.float32,
            )
            both = part if both is None else both + part
        total = both[:, DH:]
        return both[:, :DH] * (1.0 / total), top * TO_LOG2 + jnp.log2(total)

    def half(x, u):
        return x[u * rows : (u + 1) * rows]

    def finish_own(p, buf):
        value, level = attend(p, buf)
        own[:, columns(p)] = jnp.concatenate([half(value, u) for u in range(STACK)], axis=1)
        levels = half(level, 0)
        for u in range(1, STACK):
            levels = jnp.where(lane == u, half(level, u), levels)
        own_stat[p] = levels

    def finish_other(d, p, buf):
        value, level = attend(p, buf)
        size = jnp.maximum(jnp.max(jnp.abs(value), axis=1, keepdims=True), 1e-30)
        codes = jnp.round(value * (CODE_MAX / size)).astype(jnp.int32).astype(jnp.int16)
        code_out[d, :, columns(p)] = jnp.concatenate([half(codes, u) for u in range(STACK)], axis=1)
        size = jnp.broadcast_to(size * (1.0 / CODE_MAX), level.shape)
        stats = half(level, 0)
        for u in range(1, STACK):
            stats = jnp.where(lane == u, half(level, u), stats)
        for u in range(STACK):
            stats = jnp.where(lane == STACK + u, half(size, u), stats)
        stat_out[d, p] = jnp.transpose(stats)[0 : 2 * STACK]
        send_codes(d, p).start()
        send_stats(d, p).start()

    ping = chips % 2 == 0

    for i in (0, 1):
        local[i].wait()
    prepare_keys(0)
    for copy in kv_copies[:2]:
        copy.wait()
    if pair > 1:
        prepare_keys(1)
    if ping:
        find_scores(0, 0, 0)
    for i in (2, 3):
        local[i].wait()
    prepare_values(0)
    for copy in kv_copies[2:]:
        copy.wait()
    if pair > 1:
        prepare_values(1)

    def body(p, carry):
        for d in range(1, chips):
            send_query(d, p).wait_recv()
        for d in range(chips):
            buf = d % 2
            if not ping:
                find_scores(d, p, buf)
            elif d + 1 < chips:
                find_scores(d + 1, p, 1 - buf)
            else:
                find_scores(0, (p + 1) % steps, 1 - buf)
            if d == 0:
                finish_own(p, buf)
            else:
                finish_other(d, p, buf)
        return carry

    lax.fori_loop(0, steps, body, 0)

    pad[...] = jnp.zeros_like(pad)

    def combine(p, carry):
        mine = own_stat[p]
        top = mine
        got = []
        for d in range(1, chips):
            send_codes(d, p).wait_recv()
            send_stats(d, p).wait_recv()
            pad[0 : 2 * STACK] = stat_in[d, p]
            got.append(jnp.transpose(pad[...]))
            top = jnp.maximum(top, got[-1])
        mine = jnp.exp2(mine - top)
        factors = [jnp.exp2(both - top) for both in got]
        total = mine
        for factor in factors:
            total = total + factor
        inverse = 1.0 / total
        mine = mine * inverse
        factors = [factor * inverse for factor in factors]
        results = []
        for u in range(STACK):
            at = pl.ds(pl.multiple_of((p * STACK + u) * DH, DH), DH)
            result = own[:, at] * mine[:, u : u + 1]
            for d in range(1, chips):
                codes = code_in[d, :, at].astype(jnp.int32).astype(jnp.float32)
                scale = factors[d - 1][:, u : u + 1] * got[d - 1][:, STACK + u : STACK + u + 1]
                result = result + codes * scale
            results.append(result.astype(jnp.bfloat16))
        out_ref[:, columns(p)] = jnp.concatenate(results, axis=1)
        return carry

    lax.fori_loop(0, steps, combine, 0)

    for p in range(steps):
        for d in range(1, chips):
            send_query(d, p).wait_send()
            send_codes(d, p).wait_send()
            send_stats(d, p).wait_send()


def on_device(queries, new_keys, new_values, cache_keys, cache_values, valid_len, block_of):
    n = lax.axis_size("seq")
    pair = 2 if n % 2 == 0 else 1
    chips = n // pair
    rows, cols = queries.shape
    kv_cols = new_keys.shape[1]
    length = cache_keys.shape[0]
    steps = cols // (STACK * DH)
    pinned = [
        pltpu.with_memory_space_constraint(x, pltpu.HBM)
        for x in (
            queries, new_keys, new_values, cache_keys, cache_values, valid_len, block_of,
        )
    ]
    everywhere = pl.BlockSpec(memory_space=pl.ANY)
    dma = pltpu.SemaphoreType.DMA
    keys = pair * (length + rows)
    return pl.pallas_call(
        functools.partial(kernel, n, pair),
        out_shape=pltpu.VMEM((rows, cols), jnp.bfloat16),
        in_specs=[everywhere] * 7,
        out_specs=pl.BlockSpec(memory_space=pltpu.VMEM),
        scratch_shapes=[
            pltpu.VMEM((keys, kv_cols), jnp.bfloat16),
            pltpu.VMEM((keys, kv_cols), jnp.bfloat16),
            pltpu.VMEM((keys, 2 * kv_cols), jnp.bfloat16),
            pltpu.VMEM((chips, rows, cols), jnp.bfloat16),
            pltpu.VMEM((STACK * rows, keys), jnp.float32),
            pltpu.VMEM((STACK * rows, keys), jnp.float32),
            pltpu.VMEM((STACK * rows, DH), jnp.float32),
            pltpu.VMEM((STACK * rows, DH), jnp.float32),
            pltpu.VMEM((rows, cols), jnp.float32),
            pltpu.VMEM((steps, rows, DH), jnp.float32),
            pltpu.VMEM((chips, rows, cols), jnp.int16),
            pltpu.VMEM((chips, rows, cols), jnp.int16),
            pltpu.VMEM((chips, steps, 2 * STACK, rows), jnp.float32),
            pltpu.VMEM((chips, steps, 2 * STACK, rows), jnp.float32),
            pltpu.VMEM((chips, rows, pair * rows), jnp.float32),
            pltpu.VMEM((rows, DH), jnp.float32),
            pltpu.SMEM(valid_len.shape, jnp.int32),
            pltpu.SMEM(block_of.shape, jnp.int32),
            dma((7,)), dma((4,)), dma((4,)),
            dma((chips, steps)), dma((chips, steps)),
            dma((chips, steps)), dma((chips, steps)),
            dma((chips, steps)), dma((chips, steps)),
        ],
        compiler_params=pltpu.CompilerParams(
            collective_id=0, has_side_effects=True, vmem_limit_bytes=48 * 1024 * 1024,
        ),
    )(*pinned)


def solution(mesh):
    placed = (
        P(("groups", "seq"), "head"),
        P(("groups", "seq"), "head"),
        P(("groups", "seq"), "head"),
        P(("groups", "seq"), "head"),
        P(("groups", "seq"), "head"),
        P("groups"),
        P("groups"),
    )
    return jax.shard_map(
        on_device,
        mesh=mesh,
        in_specs=placed,
        out_specs=P(("groups", "seq"), "head"),
        check_vma=False,
    )
```

```python
import functools
import math

import jax
import jax.numpy as jnp
from jax import lax
from jax.experimental import pallas as pl
from jax.experimental.pallas import tpu as pltpu
from jax.sharding import PartitionSpec as P

DH = 128
GROUP = 8
NEGATIVE = -1e30
TO_LOG2 = DH ** (-0.5) * math.log2(math.e)
CODE_MAX = 32767.0
STACK = 2
TILE = 256


def kernel(
    n, pair,
    q_hbm, nk_hbm, nv_hbm, ck_hbm, cv_hbm, valid_hbm, block_hbm,
    out_ref,
    kbuf, vraw, vbuf, qbuf, score_a, score_b, top_a, top_b, own, own_stat,
    code_out, code_in, stat_out, stat_in, span_bias, pad, valid_ref, block_ref,
    loc_sem, ql_sem, kv_send, kv_recv, q_send, q_recv, r_send, r_recv, s_send, s_recv,
):
    chips = n // pair
    rows, cols = q_hbm.shape
    length, kv_cols = ck_hbm.shape
    kv_heads = kv_cols // DH
    heads = cols // DH
    steps = heads // STACK
    width = STACK * DH
    cached = pair * length
    keys = cached + pair * rows
    tiles = [(t, min(TILE, cached - t)) for t in range(0, cached, TILE)]
    tiles += [(cached + t, min(TILE, keys - cached - t)) for t in range(0, keys - cached, TILE)]
    me = lax.axis_index("seq")
    chip, core = me // pair, me % pair
    partner = chip * pair + (pair - 1 - core)

    def ahead(d):
        return ((chip + d) % chips) * pair + (pair - 1 - core)

    def behind(d):
        return ((chip + chips - d) % chips) * pair + (pair - 1 - core)

    barrier = pltpu.get_barrier_semaphore()
    others = [ahead(d) for d in range(1, chips)] + ([partner] if pair > 1 else [])
    for other in others:
        pl.semaphore_signal(barrier, inc=1, device_id={"seq": other})

    def columns(p):
        return pl.ds(pl.multiple_of(p * width, width), width)

    def local_query(p):
        return pltpu.make_async_copy(q_hbm.at[:, columns(p)], qbuf.at[0, p], ql_sem.at[p])

    sources = (ck_hbm, nk_hbm, cv_hbm, nv_hbm)

    def place(i, slot):
        buf = kbuf if i < 2 else vraw
        start, size = ((slot * length, length), (cached + slot * rows, rows))[i % 2]
        return buf.at[pl.ds(start, size), :]

    local = [
        pltpu.make_async_copy(sources[i], place(i, 0), loc_sem.at[i]) for i in range(4)
    ] + [
                pltpu.make_async_copy(valid_hbm, valid_ref, loc_sem.at[4]),
        pltpu.make_async_copy(block_hbm, block_ref, loc_sem.at[5]),
    ]
    for p in range(steps):
        local_query(p).start()
    for copy in local:
        copy.start()

    pl.semaphore_wait(barrier, len(others))

    def send_query(d, p):
        return pltpu.make_async_remote_copy(
            src_ref=qbuf.at[0, p], dst_ref=qbuf.at[d, p],
            send_sem=q_send.at[d, p], recv_sem=q_recv.at[d, p],
            device_id={"seq": ahead(d)},
        )

    def send_codes(d, p):
        return pltpu.make_async_remote_copy(
            src_ref=code_out.at[d, p], dst_ref=code_in.at[d, p],
            send_sem=r_send.at[d, p], recv_sem=r_recv.at[d, p],
            device_id={"seq": behind(d)},
        )

    def send_stats(d, p):
        return pltpu.make_async_remote_copy(
            src_ref=stat_out.at[d, p], dst_ref=stat_in.at[d, p],
            send_sem=s_send.at[d, p], recv_sem=s_recv.at[d, p],
            device_id={"seq": behind(d)},
        )

    kv_copies = []
    if pair > 1:
        kv_copies = [
            pltpu.make_async_remote_copy(
                src_ref=sources[i], dst_ref=place(i, 1),
                send_sem=kv_send.at[i], recv_sem=kv_recv.at[i],
                device_id={"seq": partner},
            )
            for i in range(4)
        ]
    for p in range(steps):
        local_query(p).wait()
        for d in range(1, chips):
            send_query(d, p).start()
        if p == 0:
            for copy in kv_copies:
                copy.start()

    local[4].wait()
    local[5].wait()
    key_owner = [me, partner][:pair]
    row_at = lax.broadcasted_iota(jnp.int32, (rows, rows), 0)
    col_at = lax.broadcasted_iota(jnp.int32, (rows, rows), 1)
    for d in range(chips):
        row_pos = block_ref[behind(d) if d else me] * rows + row_at
        for slot in range(pair):
            seen = block_ref[key_owner[slot]] * rows + col_at <= row_pos
            span_bias[d, :, slot * rows : (slot + 1) * rows] = jnp.where(seen, 0.0, NEGATIVE)

    lane = lax.broadcasted_iota(jnp.int32, (rows, DH), 1)
    slot_at = lax.broadcasted_iota(jnp.int32, (TILE, DH), 0)
    ones = jnp.ones((TILE, DH), jnp.bfloat16)

    def live_rows(slot, t):
        live = slot_at + t < valid_ref[key_owner[slot]]
        return jnp.where(live, 1.0, 0.0).astype(jnp.bfloat16)

    def prepare_keys(slot):
        first = kbuf[slot * length : slot * length + 1, :]
        for t in range(0, length, TILE):
            at = pl.ds(slot * length + t, TILE)
            live = live_rows(slot, t)
            for h in range(kv_heads):
                part = pl.ds(h * DH, DH)
                kbuf[at, part] = kbuf[at, part] * live + first[:, h * DH : (h + 1) * DH] * (ones - live)

    def prepare_values(slot):
        for t in range(0, length, TILE):
            at = pl.ds(slot * length + t, TILE)
            live = live_rows(slot, t)
            for h in range(kv_heads):
                vbuf[at, 2 * h * DH : (2 * h + 1) * DH] = vraw[at, h * DH : (h + 1) * DH] * live
                vbuf[at, (2 * h + 1) * DH : (2 * h + 2) * DH] = live
        at = pl.ds(cached + slot * rows, rows)
        for h in range(kv_heads):
            vbuf[at, 2 * h * DH : (2 * h + 1) * DH] = vraw[at, h * DH : (h + 1) * DH]
            vbuf[at, (2 * h + 1) * DH : (2 * h + 2) * DH] = jnp.ones((rows, DH), jnp.bfloat16)

    score = (score_a, score_b)
    peak = (top_a, top_b)

    def find_scores(d, p, buf):
        query = qbuf[d, p]
        stacked = jnp.concatenate([query[:, u * DH : (u + 1) * DH] for u in range(STACK)], axis=0)
        kv_at = pl.ds(pl.multiple_of(p * STACK // GROUP * DH, DH), DH)
        best = None
        for start, size in tiles:
            part = lax.dot_general(
                stacked, kbuf[start : start + size, kv_at], (((1,), (1,)), ((), ())),
                preferred_element_type=jnp.float32,
            )
            if start >= cached:
                bias = span_bias[d, :, start - cached : start - cached + size]
                part = part + jnp.concatenate([bias] * STACK, axis=0)
            score[buf][:, start : start + size] = part
            for c in range(0, size, DH):
                piece = part[:, c : c + DH]
                best = piece if best is None else jnp.maximum(best, piece)
        peak[buf][...] = jnp.broadcast_to(jnp.max(best, axis=1, keepdims=True), peak[buf].shape)

    def attend(p, buf):
        kv_at = pl.ds(pl.multiple_of(p * STACK // GROUP * (2 * DH), 2 * DH), 2 * DH)
        top = peak[buf][...]
        both = None
        for start, size in tiles:
            weights = [
                jnp.exp2((score[buf][:, start + c : start + c + DH] - top) * TO_LOG2).astype(jnp.bfloat16)
                for c in range(0, size, DH)
            ]
            part = jnp.dot(
                jnp.concatenate(weights, axis=1), vbuf[start : start + size, kv_at],
                preferred_element_type=jnp.float32,
            )
            both = part if both is None else both + part
        total = both[:, DH:]
        return both[:, :DH] * (1.0 / total), top * TO_LOG2 + jnp.log2(total)

    def half(x, u):
        return x[u * rows : (u + 1) * rows]

    def finish_own(p, buf):
        value, level = attend(p, buf)
        own[p] = jnp.concatenate([half(value, u) for u in range(STACK)], axis=1)
        levels = half(level, 0)
        for u in range(1, STACK):
            levels = jnp.where(lane == u, half(level, u), levels)
        own_stat[p] = levels

    def finish_other(d, p, buf):
        value, level = attend(p, buf)
        size = jnp.abs(half(value, 0))
        for u in range(1, STACK):
            size = jnp.maximum(size, jnp.abs(half(value, u)))
        size = jnp.maximum(jnp.max(size, axis=1, keepdims=True), 1e-30)
        scale = CODE_MAX / size
        codes = [
            jnp.round(half(value, u) * scale).astype(jnp.int32).astype(jnp.int16)
            for u in range(STACK)
        ]
        code_out[d, p] = jnp.concatenate(codes, axis=1)
        stats = size * (1.0 / CODE_MAX)
        for u in range(STACK):
            stats = jnp.where(lane == u, half(level, u), stats)
        stat_out[d, p] = jnp.transpose(stats)[0 : STACK + 1]
        send_codes(d, p).start()
        send_stats(d, p).start()

    ping = chips % 2 == 0

    for i in (0, 1):
        local[i].wait()
    prepare_keys(0)
    for copy in kv_copies[:2]:
        copy.wait()
    if pair > 1:
        prepare_keys(1)
    if ping:
        find_scores(0, 0, 0)
    for i in (2, 3):
        local[i].wait()
    prepare_values(0)
    for copy in kv_copies[2:]:
        copy.wait()
    if pair > 1:
        prepare_values(1)

    def body(p, carry):
        for d in range(1, chips):
            send_query(d, p).wait_recv()
        for d in range(chips):
            buf = d % 2
            if not ping:
                find_scores(d, p, buf)
            elif d + 1 < chips:
                find_scores(d + 1, p, 1 - buf)
            else:
                find_scores(0, (p + 1) % steps, 1 - buf)
            if d == 0:
                finish_own(p, buf)
            else:
                finish_other(d, p, buf)
        return carry

    lax.fori_loop(0, steps, body, 0)

    pad[...] = jnp.zeros_like(pad)

    def combine(p, carry):
        mine = own_stat[p]
        top = mine
        got = []
        for d in range(1, chips):
            send_codes(d, p).wait_recv()
            send_stats(d, p).wait_recv()
            pad[0 : STACK + 1] = stat_in[d, p]
            got.append(jnp.transpose(pad[...]))
            top = jnp.maximum(top, got[-1])
        mine = jnp.exp2(mine - top)
        factors = [jnp.exp2(both - top) for both in got]
        total = mine
        for factor in factors:
            total = total + factor
        inverse = 1.0 / total
        mine = mine * inverse
        factors = [factor * inverse for factor in factors]
        results = []
        for u in range(STACK):
            at = pl.ds(u * DH, DH)
            result = own[p, :, at] * mine[:, u : u + 1]
            for d in range(1, chips):
                codes = code_in[d, p, :, at].astype(jnp.int32).astype(jnp.float32)
                scale = factors[d - 1][:, u : u + 1] * got[d - 1][:, STACK : STACK + 1]
                result = result + codes * scale
            results.append(result.astype(jnp.bfloat16))
        out_ref[:, columns(p)] = jnp.concatenate(results, axis=1)
        return carry

    lax.fori_loop(0, steps, combine, 0)

    for p in range(steps):
        for d in range(1, chips):
            send_query(d, p).wait_send()
            send_codes(d, p).wait_send()
            send_stats(d, p).wait_send()


def on_device(queries, new_keys, new_values, cache_keys, cache_values, valid_len, block_of):
    n = lax.axis_size("seq")
    pair = 2 if n % 2 == 0 else 1
    chips = n // pair
    rows, cols = queries.shape
    kv_cols = new_keys.shape[1]
    length = cache_keys.shape[0]
    steps = cols // (STACK * DH)
    pinned = [
        pltpu.with_memory_space_constraint(x, pltpu.HBM)
        for x in (
            queries, new_keys, new_values, cache_keys, cache_values, valid_len, block_of,
        )
    ]
    everywhere = pl.BlockSpec(memory_space=pl.ANY)
    dma = pltpu.SemaphoreType.DMA
    keys = pair * (length + rows)
    return pl.pallas_call(
        functools.partial(kernel, n, pair),
        out_shape=pltpu.VMEM((rows, cols), jnp.bfloat16),
        in_specs=[everywhere] * 7,
        out_specs=pl.BlockSpec(memory_space=pltpu.VMEM),
        scratch_shapes=[
            pltpu.VMEM((keys, kv_cols), jnp.bfloat16),
            pltpu.VMEM((keys, kv_cols), jnp.bfloat16),
            pltpu.VMEM((keys, 2 * kv_cols), jnp.bfloat16),
            pltpu.VMEM((chips, steps, rows, STACK * DH), jnp.bfloat16),
            pltpu.VMEM((STACK * rows, keys), jnp.float32),
            pltpu.VMEM((STACK * rows, keys), jnp.float32),
            pltpu.VMEM((STACK * rows, DH), jnp.float32),
            pltpu.VMEM((STACK * rows, DH), jnp.float32),
            pltpu.VMEM((steps, rows, STACK * DH), jnp.float32),
            pltpu.VMEM((steps, rows, DH), jnp.float32),
            pltpu.VMEM((chips, steps, rows, STACK * DH), jnp.int16),
            pltpu.VMEM((chips, steps, rows, STACK * DH), jnp.int16),
            pltpu.VMEM((chips, steps, STACK + 1, rows), jnp.float32),
            pltpu.VMEM((chips, steps, STACK + 1, rows), jnp.float32),
            pltpu.VMEM((chips, rows, pair * rows), jnp.float32),
            pltpu.VMEM((rows, DH), jnp.float32),
            pltpu.SMEM(valid_len.shape, jnp.int32),
            pltpu.SMEM(block_of.shape, jnp.int32),
            dma((6,)), dma((steps,)), dma((4,)), dma((4,)),
            dma((chips, steps)), dma((chips, steps)),
            dma((chips, steps)), dma((chips, steps)),
            dma((chips, steps)), dma((chips, steps)),
        ],
        compiler_params=pltpu.CompilerParams(
            collective_id=0, has_side_effects=True, vmem_limit_bytes=48 * 1024 * 1024,
        ),
    )(*pinned)


def solution(mesh):
    placed = (
        P(("groups", "seq"), "head"),
        P(("groups", "seq"), "head"),
        P(("groups", "seq"), "head"),
        P(("groups", "seq"), "head"),
        P(("groups", "seq"), "head"),
        P("groups"),
        P("groups"),
    )
    return jax.shard_map(
        on_device,
        mesh=mesh,
        in_specs=placed,
        out_specs=P(("groups", "seq"), "head"),
        check_vma=False,
    )
```

```python
import functools
import math

import jax
import jax.numpy as jnp
from jax import lax
from jax.experimental import pallas as pl
from jax.experimental.pallas import tpu as pltpu
from jax.sharding import PartitionSpec as P

DH = 128
GROUP = 8
NEGATIVE = -1e30
TO_LOG2 = DH ** (-0.5) * math.log2(math.e)
CODE_MAX = 32767.0
STACK = 2
TILE = 256


def kernel(
    n, pair,
    q_hbm, nk_hbm, nv_hbm, ck_hbm, cv_hbm, valid_hbm, block_hbm,
    out_ref,
    kbuf, vraw, vbuf, qbuf, score_a, score_b, top_a, top_b, own, own_stat,
    code_out, code_in, stat_out, stat_in, span_bias, pad, valid_ref, block_ref,
    loc_sem, ql_sem, kv_send, kv_recv, q_send, q_recv, r_send, r_recv, s_send, s_recv,
):
    chips = n // pair
    rows, cols = q_hbm.shape
    length, kv_cols = ck_hbm.shape
    kv_heads = kv_cols // DH
    heads = cols // DH
    steps = heads // STACK
    width = STACK * DH
    cached = pair * length
    keys = cached + pair * rows
    tiles = [(t, min(TILE, cached - t)) for t in range(0, cached, TILE)]
    tiles += [(cached + t, min(TILE, keys - cached - t)) for t in range(0, keys - cached, TILE)]
    me = lax.axis_index("seq")
    chip, core = me // pair, me % pair
    partner = chip * pair + (pair - 1 - core)

    def ahead(d):
        return ((chip + d) % chips) * pair + (pair - 1 - core)

    def behind(d):
        return ((chip + chips - d) % chips) * pair + (pair - 1 - core)

    barrier = pltpu.get_barrier_semaphore()
    others = [ahead(d) for d in range(1, chips)] + ([partner] if pair > 1 else [])
    for other in others:
        pl.semaphore_signal(barrier, inc=1, device_id={"seq": other})

    def columns(p):
        return pl.ds(pl.multiple_of(p * width, width), width)

    def local_query(p):
        return pltpu.make_async_copy(q_hbm.at[:, columns(p)], qbuf.at[0, p], ql_sem.at[p])

    sources = (ck_hbm, nk_hbm, cv_hbm, nv_hbm)

    def place(i, slot):
        buf = kbuf if i < 2 else vraw
        start, size = ((slot * length, length), (cached + slot * rows, rows))[i % 2]
        return buf.at[pl.ds(start, size), :]

    local = [
        pltpu.make_async_copy(sources[i], place(i, 0), loc_sem.at[i]) for i in range(4)
    ] + [
                pltpu.make_async_copy(valid_hbm, valid_ref, loc_sem.at[4]),
        pltpu.make_async_copy(block_hbm, block_ref, loc_sem.at[5]),
    ]
    for p in range(steps):
        local_query(p).start()
    for copy in local:
        copy.start()

    pl.semaphore_wait(barrier, len(others))

    def send_query(d, p):
        return pltpu.make_async_remote_copy(
            src_ref=qbuf.at[0, p], dst_ref=qbuf.at[d, p],
            send_sem=q_send.at[d, p], recv_sem=q_recv.at[d, p],
            device_id={"seq": ahead(d)},
        )

    def send_codes(d, p):
        return pltpu.make_async_remote_copy(
            src_ref=code_out.at[d, p], dst_ref=code_in.at[d, p],
            send_sem=r_send.at[d, p], recv_sem=r_recv.at[d, p],
            device_id={"seq": behind(d)},
        )

    def send_stats(d, p):
        return pltpu.make_async_remote_copy(
            src_ref=stat_out.at[d, p], dst_ref=stat_in.at[d, p],
            send_sem=s_send.at[d, p], recv_sem=s_recv.at[d, p],
            device_id={"seq": behind(d)},
        )

    kv_copies = []
    if pair > 1:
        kv_copies = [
            pltpu.make_async_remote_copy(
                src_ref=sources[i], dst_ref=place(i, 1),
                send_sem=kv_send.at[i], recv_sem=kv_recv.at[i],
                device_id={"seq": partner},
            )
            for i in range(4)
        ]
    for p in range(steps):
        local_query(p).wait()
        for d in range(1, chips):
            send_query(d, p).start()
        if p == 0:
            for copy in kv_copies:
                copy.start()

    local[4].wait()
    local[5].wait()
    key_owner = [me, partner][:pair]
    row_at = lax.broadcasted_iota(jnp.int32, (rows, rows), 0)
    col_at = lax.broadcasted_iota(jnp.int32, (rows, rows), 1)
    for d in range(chips):
        row_pos = block_ref[behind(d) if d else me] * rows + row_at
        for slot in range(pair):
            seen = block_ref[key_owner[slot]] * rows + col_at <= row_pos
            span_bias[d, :, slot * rows : (slot + 1) * rows] = jnp.where(seen, 0.0, NEGATIVE)

    lane = lax.broadcasted_iota(jnp.int32, (rows, DH), 1)
    slot_at = lax.broadcasted_iota(jnp.int32, (TILE, DH), 0)
    ones = jnp.ones((TILE, DH), jnp.bfloat16)

    def live_rows(slot, t):
        live = slot_at + t < valid_ref[key_owner[slot]]
        return jnp.where(live, 1.0, 0.0).astype(jnp.bfloat16)

    def prepare_keys(slot):
        first = kbuf[slot * length : slot * length + 1, :]
        for t in range(0, length, TILE):
            at = pl.ds(slot * length + t, TILE)
            live = live_rows(slot, t)
            for h in range(kv_heads):
                part = pl.ds(h * DH, DH)
                kbuf[at, part] = kbuf[at, part] * live + first[:, h * DH : (h + 1) * DH] * (ones - live)

    def prepare_values(slot):
        for t in range(0, length, TILE):
            at = pl.ds(slot * length + t, TILE)
            live = live_rows(slot, t)
            for h in range(kv_heads):
                vbuf[at, 2 * h * DH : (2 * h + 1) * DH] = vraw[at, h * DH : (h + 1) * DH] * live
                vbuf[at, (2 * h + 1) * DH : (2 * h + 2) * DH] = live
        at = pl.ds(cached + slot * rows, rows)
        for h in range(kv_heads):
            vbuf[at, 2 * h * DH : (2 * h + 1) * DH] = vraw[at, h * DH : (h + 1) * DH]
            vbuf[at, (2 * h + 1) * DH : (2 * h + 2) * DH] = jnp.ones((rows, DH), jnp.bfloat16)

    score = (score_a, score_b)
    peak = (top_a, top_b)

    def find_scores(d, p, buf):
        query = qbuf[d, p]
        stacked = jnp.concatenate([query[:, u * DH : (u + 1) * DH] for u in range(STACK)], axis=0)
        kv_at = pl.ds(pl.multiple_of(p * STACK // GROUP * DH, DH), DH)
        best = None
        for start, size in tiles:
            part = lax.dot_general(
                stacked, kbuf[start : start + size, kv_at], (((1,), (1,)), ((), ())),
                preferred_element_type=jnp.float32,
            )
            if start >= cached:
                bias = span_bias[d, :, start - cached : start - cached + size]
                part = part + jnp.concatenate([bias] * STACK, axis=0)
            score[buf][:, start : start + size] = part
            for c in range(0, size, DH):
                piece = part[:, c : c + DH]
                best = piece if best is None else jnp.maximum(best, piece)
        peak[buf][...] = jnp.broadcast_to(jnp.max(best, axis=1, keepdims=True), peak[buf].shape)

    def attend(p, buf):
        kv_at = pl.ds(pl.multiple_of(p * STACK // GROUP * (2 * DH), 2 * DH), 2 * DH)
        top = peak[buf][...]
        both = None
        for start, size in tiles:
            weights = [
                jnp.exp2((score[buf][:, start + c : start + c + DH] - top) * TO_LOG2).astype(jnp.bfloat16)
                for c in range(0, size, DH)
            ]
            part = jnp.dot(
                jnp.concatenate(weights, axis=1), vbuf[start : start + size, kv_at],
                preferred_element_type=jnp.float32,
            )
            both = part if both is None else both + part
        total = both[:, DH:]
        return both[:, :DH] * (1.0 / total), top * TO_LOG2 + jnp.log2(total)

    def half(x, u):
        return x[u * rows : (u + 1) * rows]

    def finish_own(p, buf):
        value, level = attend(p, buf)
        own[p] = jnp.concatenate([half(value, u) for u in range(STACK)], axis=1)
        levels = half(level, 0)
        for u in range(1, STACK):
            levels = jnp.where(lane == u, half(level, u), levels)
        own_stat[p] = levels

    def finish_other(d, p, buf):
        value, level = attend(p, buf)
        size = jnp.abs(half(value, 0))
        for u in range(1, STACK):
            size = jnp.maximum(size, jnp.abs(half(value, u)))
        size = jnp.maximum(jnp.max(size, axis=1, keepdims=True), 1e-30)
        scale = CODE_MAX / size
        codes = [
            jnp.round(half(value, u) * scale).astype(jnp.int32).astype(jnp.int16)
            for u in range(STACK)
        ]
        code_out[d, p] = jnp.concatenate(codes, axis=1)
        stats = size * (1.0 / CODE_MAX)
        for u in range(STACK):
            stats = jnp.where(lane == u, half(level, u), stats)
        stat_out[d, p] = jnp.transpose(stats)[0 : STACK + 1]
        send_stats(d, p).start()
        send_codes(d, p).start()

    ping = chips % 2 == 0

    for i in (0, 1):
        local[i].wait()
    prepare_keys(0)
    for copy in kv_copies[:2]:
        copy.wait()
    if pair > 1:
        prepare_keys(1)
    if ping:
        find_scores(0, 0, 0)
    for i in (2, 3):
        local[i].wait()
    prepare_values(0)
    for copy in kv_copies[2:]:
        copy.wait()
    if pair > 1:
        prepare_values(1)

    def body(p, carry):
        for d in range(1, chips):
            send_query(d, p).wait_recv()
        for d in range(chips):
            buf = d % 2
            if not ping:
                find_scores(d, p, buf)
            elif d + 1 < chips:
                find_scores(d + 1, p, 1 - buf)
            else:
                find_scores(0, (p + 1) % steps, 1 - buf)
            if d == 0:
                finish_own(p, buf)
            else:
                finish_other(d, p, buf)
        return carry

    lax.fori_loop(0, steps, body, 0)

    pad[...] = jnp.zeros_like(pad)

    def combine(p, carry):
        mine = own_stat[p]
        top = mine
        got = []
        for d in range(1, chips):
            send_stats(d, p).wait_recv()
            pad[0 : STACK + 1] = stat_in[d, p]
            got.append(jnp.transpose(pad[...]))
            top = jnp.maximum(top, got[-1])
        mine = jnp.exp2(mine - top)
        factors = [jnp.exp2(both - top) for both in got]
        total = mine
        for factor in factors:
            total = total + factor
        inverse = 1.0 / total
        mine = mine * inverse
        factors = [factor * inverse for factor in factors]
        scales = [
            [factors[d - 1][:, u : u + 1] * got[d - 1][:, STACK : STACK + 1] for d in range(1, chips)]
            for u in range(STACK)
        ]
        results = [own[p, :, u * DH : (u + 1) * DH] * mine[:, u : u + 1] for u in range(STACK)]
        for d in range(1, chips):
            send_codes(d, p).wait_recv()
            for u in range(STACK):
                codes = code_in[d, p, :, u * DH : (u + 1) * DH].astype(jnp.int32).astype(jnp.float32)
                results[u] = results[u] + codes * scales[u][d - 1]
        results = [result.astype(jnp.bfloat16) for result in results]
        out_ref[:, columns(p)] = jnp.concatenate(results, axis=1)
        return carry

    lax.fori_loop(0, steps, combine, 0)

    for p in range(steps):
        for d in range(1, chips):
            send_query(d, p).wait_send()
            send_codes(d, p).wait_send()
            send_stats(d, p).wait_send()


def on_device(queries, new_keys, new_values, cache_keys, cache_values, valid_len, block_of):
    n = lax.axis_size("seq")
    pair = 2 if n % 2 == 0 else 1
    chips = n // pair
    rows, cols = queries.shape
    kv_cols = new_keys.shape[1]
    length = cache_keys.shape[0]
    steps = cols // (STACK * DH)
    pinned = [
        pltpu.with_memory_space_constraint(x, pltpu.HBM)
        for x in (
            queries, new_keys, new_values, cache_keys, cache_values, valid_len, block_of,
        )
    ]
    everywhere = pl.BlockSpec(memory_space=pl.ANY)
    dma = pltpu.SemaphoreType.DMA
    keys = pair * (length + rows)
    return pl.pallas_call(
        functools.partial(kernel, n, pair),
        out_shape=pltpu.VMEM((rows, cols), jnp.bfloat16),
        in_specs=[everywhere] * 7,
        out_specs=pl.BlockSpec(memory_space=pltpu.VMEM),
        scratch_shapes=[
            pltpu.VMEM((keys, kv_cols), jnp.bfloat16),
            pltpu.VMEM((keys, kv_cols), jnp.bfloat16),
            pltpu.VMEM((keys, 2 * kv_cols), jnp.bfloat16),
            pltpu.VMEM((chips, steps, rows, STACK * DH), jnp.bfloat16),
            pltpu.VMEM((STACK * rows, keys), jnp.float32),
            pltpu.VMEM((STACK * rows, keys), jnp.float32),
            pltpu.VMEM((STACK * rows, DH), jnp.float32),
            pltpu.VMEM((STACK * rows, DH), jnp.float32),
            pltpu.VMEM((steps, rows, STACK * DH), jnp.float32),
            pltpu.VMEM((steps, rows, DH), jnp.float32),
            pltpu.VMEM((chips, steps, rows, STACK * DH), jnp.int16),
            pltpu.VMEM((chips, steps, rows, STACK * DH), jnp.int16),
            pltpu.VMEM((chips, steps, STACK + 1, rows), jnp.float32),
            pltpu.VMEM((chips, steps, STACK + 1, rows), jnp.float32),
            pltpu.VMEM((chips, rows, pair * rows), jnp.float32),
            pltpu.VMEM((rows, DH), jnp.float32),
            pltpu.SMEM(valid_len.shape, jnp.int32),
            pltpu.SMEM(block_of.shape, jnp.int32),
            dma((6,)), dma((steps,)), dma((4,)), dma((4,)),
            dma((chips, steps)), dma((chips, steps)),
            dma((chips, steps)), dma((chips, steps)),
            dma((chips, steps)), dma((chips, steps)),
        ],
        compiler_params=pltpu.CompilerParams(
            collective_id=0, has_side_effects=True, vmem_limit_bytes=48 * 1024 * 1024,
        ),
    )(*pinned)


def solution(mesh):
    placed = (
        P(("groups", "seq"), "head"),
        P(("groups", "seq"), "head"),
        P(("groups", "seq"), "head"),
        P(("groups", "seq"), "head"),
        P(("groups", "seq"), "head"),
        P("groups"),
        P("groups"),
    )
    return jax.shard_map(
        on_device,
        mesh=mesh,
        in_specs=placed,
        out_specs=P(("groups", "seq"), "head"),
        check_vma=False,
    )
```

```python
import functools
import math

import jax
import jax.numpy as jnp
from jax import lax
from jax.experimental import pallas as pl
from jax.experimental.pallas import tpu as pltpu
from jax.sharding import PartitionSpec as P

DH = 128
GROUP = 8
NEGATIVE = -1e30
TO_LOG2 = DH ** (-0.5) * math.log2(math.e)
CODE_MAX = 32767.0
STACK = 2
TILE = 256


def kernel(
    n, pair,
    q_hbm, nk_hbm, nv_hbm, ck_hbm, cv_hbm, valid_hbm, block_hbm,
    out_ref,
    kbuf, vraw, vbuf, qbuf, score_a, score_b, top_a, top_b, own, own_stat,
    code_out, code_in, stat_out, stat_in, span_bias, repeat, pad, valid_ref, block_ref,
    loc_sem, ql_sem, kv_send, kv_recv, q_send, q_recv, r_send, r_recv, s_send, s_recv,
):
    chips = n // pair
    rows, cols = q_hbm.shape
    length, kv_cols = ck_hbm.shape
    kv_heads = kv_cols // DH
    heads = cols // DH
    steps = heads // STACK
    width = STACK * DH
    cached = pair * length
    keys = cached + pair * rows
    tiles = [(t, min(TILE, cached - t)) for t in range(0, cached, TILE)]
    tiles += [(cached + t, min(TILE, keys - cached - t)) for t in range(0, keys - cached, TILE)]
    me = lax.axis_index("seq")
    chip, core = me // pair, me % pair
    partner = chip * pair + (pair - 1 - core)

    def ahead(d):
        return ((chip + d) % chips) * pair + (pair - 1 - core)

    def behind(d):
        return ((chip + chips - d) % chips) * pair + (pair - 1 - core)

    barrier = pltpu.get_barrier_semaphore()
    others = [ahead(d) for d in range(1, chips)] + ([partner] if pair > 1 else [])
    for other in others:
        pl.semaphore_signal(barrier, inc=1, device_id={"seq": other})

    def columns(p):
        return pl.ds(pl.multiple_of(p * width, width), width)

    def local_query(p):
        return pltpu.make_async_copy(q_hbm.at[:, columns(p)], qbuf.at[0, p], ql_sem.at[p])

    sources = (ck_hbm, nk_hbm, cv_hbm, nv_hbm)

    def place(i, slot):
        buf = kbuf if i < 2 else vraw
        start, size = ((slot * length, length), (cached + slot * rows, rows))[i % 2]
        return buf.at[pl.ds(start, size), :]

    local = [
        pltpu.make_async_copy(sources[i], place(i, 0), loc_sem.at[i]) for i in range(4)
    ] + [
                pltpu.make_async_copy(valid_hbm, valid_ref, loc_sem.at[4]),
        pltpu.make_async_copy(block_hbm, block_ref, loc_sem.at[5]),
    ]
    for p in range(steps):
        local_query(p).start()
    for copy in local:
        copy.start()

    pl.semaphore_wait(barrier, len(others))

    def send_query(d, p):
        return pltpu.make_async_remote_copy(
            src_ref=qbuf.at[0, p], dst_ref=qbuf.at[d, p],
            send_sem=q_send.at[d, p], recv_sem=q_recv.at[d, p],
            device_id={"seq": ahead(d)},
        )

    def send_codes(d, p):
        return pltpu.make_async_remote_copy(
            src_ref=code_out.at[d, p], dst_ref=code_in.at[d, p],
            send_sem=r_send.at[d, p], recv_sem=r_recv.at[d, p],
            device_id={"seq": behind(d)},
        )

    def send_stats(d, p):
        return pltpu.make_async_remote_copy(
            src_ref=stat_out.at[d, p], dst_ref=stat_in.at[d, p],
            send_sem=s_send.at[d, p], recv_sem=s_recv.at[d, p],
            device_id={"seq": behind(d)},
        )

    kv_copies = []
    if pair > 1:
        kv_copies = [
            pltpu.make_async_remote_copy(
                src_ref=sources[i], dst_ref=place(i, 1),
                send_sem=kv_send.at[i], recv_sem=kv_recv.at[i],
                device_id={"seq": partner},
            )
            for i in range(4)
        ]
    for p in range(steps):
        local_query(p).wait()
        for d in range(1, chips):
            send_query(d, p).start()
        if p == 0:
            for copy in kv_copies:
                copy.start()

    local[4].wait()
    local[5].wait()
    key_owner = [me, partner][:pair]
    row_at = lax.broadcasted_iota(jnp.int32, (rows, rows), 0)
    col_at = lax.broadcasted_iota(jnp.int32, (rows, rows), 1)
    for d in range(chips):
        row_pos = block_ref[behind(d) if d else me] * rows + row_at
        for slot in range(pair):
            seen = block_ref[key_owner[slot]] * rows + col_at <= row_pos
            span_bias[d, :, slot * rows : (slot + 1) * rows] = jnp.where(seen, 0.0, NEGATIVE)

    lane = lax.broadcasted_iota(jnp.int32, (rows, DH), 1)
    slot_at = lax.broadcasted_iota(jnp.int32, (TILE, DH), 0)
    ones = jnp.ones((TILE, DH), jnp.bfloat16)

    def live_rows(slot, t):
        live = slot_at + t < valid_ref[key_owner[slot]]
        return jnp.where(live, 1.0, 0.0).astype(jnp.bfloat16)

    def prepare_keys(slot):
        first = kbuf[slot * length : slot * length + 1, :]
        for t in range(0, length, TILE):
            at = pl.ds(slot * length + t, TILE)
            live = live_rows(slot, t)
            for h in range(kv_heads):
                part = pl.ds(h * DH, DH)
                kbuf[at, part] = kbuf[at, part] * live + first[:, h * DH : (h + 1) * DH] * (ones - live)

    def prepare_values(slot):
        for t in range(0, length, TILE):
            at = pl.ds(slot * length + t, TILE)
            live = live_rows(slot, t)
            for h in range(kv_heads):
                vbuf[at, 2 * h * DH : (2 * h + 1) * DH] = vraw[at, h * DH : (h + 1) * DH] * live
                vbuf[at, (2 * h + 1) * DH : (2 * h + 2) * DH] = live
        at = pl.ds(cached + slot * rows, rows)
        for h in range(kv_heads):
            vbuf[at, 2 * h * DH : (2 * h + 1) * DH] = vraw[at, h * DH : (h + 1) * DH]
            vbuf[at, (2 * h + 1) * DH : (2 * h + 2) * DH] = jnp.ones((rows, DH), jnp.bfloat16)

    for slot in range(pair):
        copies = (length - valid_ref[key_owner[slot]]).astype(jnp.float32)
        repeat[slot] = jnp.where(lane[0:8] == 0, 1.0 - copies, 1.0)

    score = (score_a, score_b)
    peak = (top_a, top_b)

    def find_scores(d, p, buf):
        query = qbuf[d, p]
        stacked = jnp.concatenate([query[:, u * DH : (u + 1) * DH] for u in range(STACK)], axis=0)
        kv_at = pl.ds(pl.multiple_of(p * STACK // GROUP * DH, DH), DH)
        best = None
        for start, size in tiles:
            part = lax.dot_general(
                stacked, kbuf[start : start + size, kv_at], (((1,), (1,)), ((), ())),
                preferred_element_type=jnp.float32,
            )
            if start >= cached:
                bias = span_bias[d, :, start - cached : start - cached + size]
                part = part + jnp.concatenate([bias] * STACK, axis=0)
            score[buf][:, start : start + size] = part
            for c in range(0, size, DH):
                piece = part[:, c : c + DH]
                best = piece if best is None else jnp.maximum(best, piece)
        peak[buf][...] = jnp.broadcast_to(jnp.max(best, axis=1, keepdims=True), peak[buf].shape)

    def attend(p, buf):
        kv_at = pl.ds(pl.multiple_of(p * STACK // GROUP * (2 * DH), 2 * DH), 2 * DH)
        top = peak[buf][...]
        value = total = None
        for start, size in tiles:
            rounded = []
            for c in range(start, start + size, DH):
                weights = jnp.exp2((score[buf][:, c : c + DH] - top) * TO_LOG2)
                rounded.append(weights.astype(jnp.bfloat16))
                if c < cached and c % length == 0:
                    weights = weights * repeat[c // length, 0:1]
                total = weights if total is None else total + weights
            part = jnp.dot(
                jnp.concatenate(rounded, axis=1), vbuf[start : start + size, kv_at],
                preferred_element_type=jnp.float32,
            )
            value = part if value is None else value + part
        total = jnp.sum(total, axis=1, keepdims=True)
        return value[:, :DH] * (1.0 / total), top * TO_LOG2 + jnp.log2(total)

    def half(x, u):
        return x[u * rows : (u + 1) * rows]

    def finish_own(p, buf):
        value, level = attend(p, buf)
        own[p] = jnp.concatenate([half(value, u) for u in range(STACK)], axis=1)
        levels = half(level, 0)
        for u in range(1, STACK):
            levels = jnp.where(lane == u, half(level, u), levels)
        own_stat[p] = levels

    def finish_other(d, p, buf):
        value, level = attend(p, buf)
        size = jnp.abs(half(value, 0))
        for u in range(1, STACK):
            size = jnp.maximum(size, jnp.abs(half(value, u)))
        size = jnp.maximum(jnp.max(size, axis=1, keepdims=True), 1e-30)
        scale = CODE_MAX / size
        codes = [
            jnp.round(half(value, u) * scale).astype(jnp.int32).astype(jnp.int16)
            for u in range(STACK)
        ]
        code_out[d, p] = jnp.concatenate(codes, axis=1)
        stats = size * (1.0 / CODE_MAX)
        for u in range(STACK):
            stats = jnp.where(lane == u, half(level, u), stats)
        stat_out[d, p] = jnp.transpose(stats)[0 : STACK + 1]
        send_stats(d, p).start()
        send_codes(d, p).start()

    ping = chips % 2 == 0

    for i in (0, 1):
        local[i].wait()
    prepare_keys(0)
    for copy in kv_copies[:2]:
        copy.wait()
    if pair > 1:
        prepare_keys(1)
    if ping:
        find_scores(0, 0, 0)
    for i in (2, 3):
        local[i].wait()
    prepare_values(0)
    for copy in kv_copies[2:]:
        copy.wait()
    if pair > 1:
        prepare_values(1)

    def body(p, carry):
        for d in range(1, chips):
            send_query(d, p).wait_recv()
        for d in range(chips):
            buf = d % 2
            if not ping:
                find_scores(d, p, buf)
            elif d + 1 < chips:
                find_scores(d + 1, p, 1 - buf)
            else:
                find_scores(0, (p + 1) % steps, 1 - buf)
            if d == 0:
                finish_own(p, buf)
            else:
                finish_other(d, p, buf)
        return carry

    lax.fori_loop(0, steps, body, 0)

    pad[...] = jnp.zeros_like(pad)

    def combine(p, carry):
        mine = own_stat[p]
        top = mine
        got = []
        for d in range(1, chips):
            send_stats(d, p).wait_recv()
            pad[0 : STACK + 1] = stat_in[d, p]
            got.append(jnp.transpose(pad[...]))
            top = jnp.maximum(top, got[-1])
        mine = jnp.exp2(mine - top)
        factors = [jnp.exp2(both - top) for both in got]
        total = mine
        for factor in factors:
            total = total + factor
        inverse = 1.0 / total
        mine = mine * inverse
        factors = [factor * inverse for factor in factors]
        scales = [
            [factors[d - 1][:, u : u + 1] * got[d - 1][:, STACK : STACK + 1] for d in range(1, chips)]
            for u in range(STACK)
        ]
        results = [own[p, :, u * DH : (u + 1) * DH] * mine[:, u : u + 1] for u in range(STACK)]
        for d in range(1, chips):
            send_codes(d, p).wait_recv()
            for u in range(STACK):
                codes = code_in[d, p, :, u * DH : (u + 1) * DH].astype(jnp.int32).astype(jnp.float32)
                results[u] = results[u] + codes * scales[u][d - 1]
        results = [result.astype(jnp.bfloat16) for result in results]
        out_ref[:, columns(p)] = jnp.concatenate(results, axis=1)
        return carry

    lax.fori_loop(0, steps, combine, 0)

    for p in range(steps):
        for d in range(1, chips):
            send_query(d, p).wait_send()
            send_codes(d, p).wait_send()
            send_stats(d, p).wait_send()


def on_device(queries, new_keys, new_values, cache_keys, cache_values, valid_len, block_of):
    n = lax.axis_size("seq")
    pair = 2 if n % 2 == 0 else 1
    chips = n // pair
    rows, cols = queries.shape
    kv_cols = new_keys.shape[1]
    length = cache_keys.shape[0]
    steps = cols // (STACK * DH)
    pinned = [
        pltpu.with_memory_space_constraint(x, pltpu.HBM)
        for x in (
            queries, new_keys, new_values, cache_keys, cache_values, valid_len, block_of,
        )
    ]
    everywhere = pl.BlockSpec(memory_space=pl.ANY)
    dma = pltpu.SemaphoreType.DMA
    keys = pair * (length + rows)
    return pl.pallas_call(
        functools.partial(kernel, n, pair),
        out_shape=pltpu.VMEM((rows, cols), jnp.bfloat16),
        in_specs=[everywhere] * 7,
        out_specs=pl.BlockSpec(memory_space=pltpu.VMEM),
        scratch_shapes=[
            pltpu.VMEM((keys, kv_cols), jnp.bfloat16),
            pltpu.VMEM((keys, kv_cols), jnp.bfloat16),
            pltpu.VMEM((keys, 2 * kv_cols), jnp.bfloat16),
            pltpu.VMEM((chips, steps, rows, STACK * DH), jnp.bfloat16),
            pltpu.VMEM((STACK * rows, keys), jnp.float32),
            pltpu.VMEM((STACK * rows, keys), jnp.float32),
            pltpu.VMEM((STACK * rows, DH), jnp.float32),
            pltpu.VMEM((STACK * rows, DH), jnp.float32),
            pltpu.VMEM((steps, rows, STACK * DH), jnp.float32),
            pltpu.VMEM((steps, rows, DH), jnp.float32),
            pltpu.VMEM((chips, steps, rows, STACK * DH), jnp.int16),
            pltpu.VMEM((chips, steps, rows, STACK * DH), jnp.int16),
            pltpu.VMEM((chips, steps, STACK + 1, rows), jnp.float32),
            pltpu.VMEM((chips, steps, STACK + 1, rows), jnp.float32),
            pltpu.VMEM((chips, rows, pair * rows), jnp.float32),
            pltpu.VMEM((pair, 8, DH), jnp.float32),
            pltpu.VMEM((rows, DH), jnp.float32),
            pltpu.SMEM(valid_len.shape, jnp.int32),
            pltpu.SMEM(block_of.shape, jnp.int32),
            dma((6,)), dma((steps,)), dma((4,)), dma((4,)),
            dma((chips, steps)), dma((chips, steps)),
            dma((chips, steps)), dma((chips, steps)),
            dma((chips, steps)), dma((chips, steps)),
        ],
        compiler_params=pltpu.CompilerParams(
            collective_id=0, has_side_effects=True, vmem_limit_bytes=48 * 1024 * 1024,
        ),
    )(*pinned)


def solution(mesh):
    placed = (
        P(("groups", "seq"), "head"),
        P(("groups", "seq"), "head"),
        P(("groups", "seq"), "head"),
        P(("groups", "seq"), "head"),
        P(("groups", "seq"), "head"),
        P("groups"),
        P("groups"),
    )
    return jax.shard_map(
        on_device,
        mesh=mesh,
        in_specs=placed,
        out_specs=P(("groups", "seq"), "head"),
        check_vma=False,
    )
```

```python
import functools
import math

import jax
import jax.numpy as jnp
from jax import lax
from jax.experimental import pallas as pl
from jax.experimental.pallas import tpu as pltpu
from jax.sharding import PartitionSpec as P

DH = 128
GROUP = 8
NEGATIVE = -1e30
TO_LOG2 = DH ** (-0.5) * math.log2(math.e)
CODE_MAX = 32767.0
STACK = 2
TILE = 256


def kernel(
    n, pair,
    q_hbm, nk_hbm, nv_hbm, ck_hbm, cv_hbm, valid_hbm, block_hbm,
    out_ref,
    kbuf, vraw, vbuf, qbuf, score_a, score_b, top_a, top_b, own, own_stat,
    code_out, code_in, stat_out, stat_in, span_bias, repeat, pad, valid_ref, block_ref,
    loc_sem, ql_sem, kv_send, kv_recv, q_send, q_recv, r_send, r_recv, s_send, s_recv,
):
    chips = n // pair
    rows, cols = q_hbm.shape
    length, kv_cols = ck_hbm.shape
    kv_heads = kv_cols // DH
    heads = cols // DH
    steps = heads // STACK
    width = STACK * DH
    cached = pair * length
    keys = cached + pair * rows
    tiles = [(t, min(TILE, cached - t)) for t in range(0, cached, TILE)]
    tiles += [(cached + t, min(TILE, keys - cached - t)) for t in range(0, keys - cached, TILE)]
    me = lax.axis_index("seq")
    chip, core = me // pair, me % pair
    partner = chip * pair + (pair - 1 - core)

    def ahead(d):
        return ((chip + d) % chips) * pair + (pair - 1 - core)

    def behind(d):
        return ((chip + chips - d) % chips) * pair + (pair - 1 - core)

    barrier = pltpu.get_barrier_semaphore()
    others = [ahead(d) for d in range(1, chips)] + ([partner] if pair > 1 else [])
    for other in others:
        pl.semaphore_signal(barrier, inc=1, device_id={"seq": other})

    def columns(p):
        return pl.ds(pl.multiple_of(p * width, width), width)

    def local_query(p):
        return pltpu.make_async_copy(q_hbm.at[:, columns(p)], qbuf.at[0, p], ql_sem.at[min(p, 1)])

    def await_bytes(ref, sem):
        pltpu.make_async_copy(ref, ref, sem).wait()

    sources = (ck_hbm, nk_hbm, cv_hbm, nv_hbm)

    def place(i, slot):
        buf = kbuf if i < 2 else vraw
        start, size = ((slot * length, length), (cached + slot * rows, rows))[i % 2]
        return buf.at[pl.ds(start, size), :]

    local = [
        pltpu.make_async_copy(sources[i], place(i, 0), loc_sem.at[i // 2]) for i in range(4)
    ] + [
        pltpu.make_async_copy(valid_hbm, valid_ref, loc_sem.at[2]),
        pltpu.make_async_copy(block_hbm, block_ref, loc_sem.at[3]),
    ]
    for p in range(steps):
        local_query(p).start()
    for copy in local:
        copy.start()

    pl.semaphore_wait(barrier, len(others))

    def send_query(d, p, count=1):
        return pltpu.make_async_remote_copy(
            src_ref=qbuf.at[0, pl.ds(p, count)], dst_ref=qbuf.at[d, pl.ds(p, count)],
            send_sem=q_send.at[d - 1], recv_sem=q_recv.at[d - 1, p // 2 + 1 if count == 2 else p],
            device_id={"seq": ahead(d)},
        )

    def code_slot(p, count):
        return {1: p - (steps - 2) // 2, 2: p // 2}.get(count, 0)

    def send_codes(d, p, count=1):
        return pltpu.make_async_remote_copy(
            src_ref=code_out.at[d, pl.ds(p, count)], dst_ref=code_in.at[d, pl.ds(p, count)],
            send_sem=r_send.at[d - 1], recv_sem=r_recv.at[d - 1, code_slot(p, count)],
            device_id={"seq": behind(d)},
        )

    def send_stats(d, p, count=1):
        return pltpu.make_async_remote_copy(
            src_ref=stat_out.at[d, pl.ds(p, count)], dst_ref=stat_in.at[d, pl.ds(p, count)],
            send_sem=s_send.at[d - 1], recv_sem=s_recv.at[d - 1, code_slot(p, count)],
            device_id={"seq": behind(d)},
        )

    kv_copies = []
    if pair > 1:
        kv_copies = [
            pltpu.make_async_remote_copy(
                src_ref=sources[i], dst_ref=place(i, 1),
                send_sem=kv_send.at[0], recv_sem=kv_recv.at[i // 2],
                device_id={"seq": partner},
            )
            for i in range(4)
        ]
    local_query(0).wait()
    for d in range(1, chips):
        send_query(d, 0).start()
    for copy in kv_copies:
        copy.start()
    await_bytes(qbuf.at[0, pl.ds(1, steps - 1)], ql_sem.at[1])
    for first, count in [(1, 1)] + [(p, 2) for p in range(2, steps, 2)]:
        for d in range(1, chips):
            send_query(d, first, count).start()

    local[4].wait()
    local[5].wait()
    key_owner = [me, partner][:pair]
    row_at = lax.broadcasted_iota(jnp.int32, (rows, rows), 0)
    col_at = lax.broadcasted_iota(jnp.int32, (rows, rows), 1)
    for d in range(chips):
        row_pos = block_ref[behind(d) if d else me] * rows + row_at
        for slot in range(pair):
            seen = block_ref[key_owner[slot]] * rows + col_at <= row_pos
            span_bias[d, :, slot * rows : (slot + 1) * rows] = jnp.where(seen, 0.0, NEGATIVE)

    lane = lax.broadcasted_iota(jnp.int32, (rows, DH), 1)
    slot_at = lax.broadcasted_iota(jnp.int32, (TILE, DH), 0)
    ones = jnp.ones((TILE, DH), jnp.bfloat16)

    def live_rows(slot, t):
        live = slot_at + t < valid_ref[key_owner[slot]]
        return jnp.where(live, 1.0, 0.0).astype(jnp.bfloat16)

    def prepare_keys(slot):
        first = kbuf[slot * length : slot * length + 1, :]
        for t in range(0, length, TILE):
            at = pl.ds(slot * length + t, TILE)
            live = live_rows(slot, t)
            for h in range(kv_heads):
                part = pl.ds(h * DH, DH)
                kbuf[at, part] = kbuf[at, part] * live + first[:, h * DH : (h + 1) * DH] * (ones - live)

    def prepare_values(slot):
        for t in range(0, length, TILE):
            at = pl.ds(slot * length + t, TILE)
            live = live_rows(slot, t)
            for h in range(kv_heads):
                vbuf[at, 2 * h * DH : (2 * h + 1) * DH] = vraw[at, h * DH : (h + 1) * DH] * live
                vbuf[at, (2 * h + 1) * DH : (2 * h + 2) * DH] = live
        at = pl.ds(cached + slot * rows, rows)
        for h in range(kv_heads):
            vbuf[at, 2 * h * DH : (2 * h + 1) * DH] = vraw[at, h * DH : (h + 1) * DH]
            vbuf[at, (2 * h + 1) * DH : (2 * h + 2) * DH] = jnp.ones((rows, DH), jnp.bfloat16)

    for slot in range(pair):
        copies = (length - valid_ref[key_owner[slot]]).astype(jnp.float32)
        repeat[slot] = jnp.where(lane[0:8] == 0, 1.0 - copies, 1.0)

    score = (score_a, score_b)
    peak = (top_a, top_b)

    def find_scores(d, p, buf):
        query = qbuf[d, p]
        stacked = jnp.concatenate([query[:, u * DH : (u + 1) * DH] for u in range(STACK)], axis=0)
        kv_at = pl.ds(pl.multiple_of(p * STACK // GROUP * DH, DH), DH)
        best = None
        for start, size in tiles:
            part = lax.dot_general(
                stacked, kbuf[start : start + size, kv_at], (((1,), (1,)), ((), ())),
                preferred_element_type=jnp.float32,
            )
            if start >= cached:
                bias = span_bias[d, :, start - cached : start - cached + size]
                part = part + jnp.concatenate([bias] * STACK, axis=0)
            score[buf][:, start : start + size] = part
            for c in range(0, size, DH):
                piece = part[:, c : c + DH]
                best = piece if best is None else jnp.maximum(best, piece)
        peak[buf][...] = jnp.broadcast_to(jnp.max(best, axis=1, keepdims=True), peak[buf].shape)

    def attend(p, buf):
        kv_at = pl.ds(pl.multiple_of(p * STACK // GROUP * (2 * DH), 2 * DH), 2 * DH)
        top = peak[buf][...]
        value = total = None
        for start, size in tiles:
            rounded = []
            for c in range(start, start + size, DH):
                weights = jnp.exp2((score[buf][:, c : c + DH] - top) * TO_LOG2)
                rounded.append(weights.astype(jnp.bfloat16))
                if c < cached and c % length == 0:
                    weights = weights * repeat[c // length, 0:1]
                total = weights if total is None else total + weights
            part = jnp.dot(
                jnp.concatenate(rounded, axis=1), vbuf[start : start + size, kv_at],
                preferred_element_type=jnp.float32,
            )
            value = part if value is None else value + part
        total = jnp.sum(total, axis=1, keepdims=True)
        return value[:, :DH] * (1.0 / total), top * TO_LOG2 + jnp.log2(total)

    def half(x, u):
        return x[u * rows : (u + 1) * rows]

    def finish_own(p, buf):
        value, level = attend(p, buf)
        own[p] = jnp.concatenate([half(value, u) for u in range(STACK)], axis=1)
        levels = half(level, 0)
        for u in range(1, STACK):
            levels = jnp.where(lane == u, half(level, u), levels)
        own_stat[p] = levels

    def finish_other(d, p, buf):
        value, level = attend(p, buf)
        size = jnp.abs(half(value, 0))
        for u in range(1, STACK):
            size = jnp.maximum(size, jnp.abs(half(value, u)))
        size = jnp.maximum(jnp.max(size, axis=1, keepdims=True), 1e-30)
        scale = CODE_MAX / size
        codes = [
            jnp.round(half(value, u) * scale).astype(jnp.int32).astype(jnp.int16)
            for u in range(STACK)
        ]
        code_out[d, p] = jnp.concatenate(codes, axis=1)
        stats = size * (1.0 / CODE_MAX)
        for u in range(STACK):
            stats = jnp.where(lane == u, half(level, u), stats)
        stat_out[d, p] = jnp.transpose(stats)[0 : STACK + 1]

        @pl.when(p >= steps - 2)
        def _():
            send_stats(d, p).start()
            send_codes(d, p).start()

        @pl.when((p < steps - 2) & (p % 2 == 1))
        def _():
            send_stats(d, p - 1, 2).start()
            send_codes(d, p - 1, 2).start()

    ping = chips % 2 == 0

    share = pl.ds(0, length + rows)
    await_bytes(kbuf.at[share], loc_sem.at[0])
    prepare_keys(0)
    if pair > 1:
        await_bytes(kbuf.at[share], kv_recv.at[0])
        prepare_keys(1)
    if ping:
        find_scores(0, 0, 0)
    await_bytes(vraw.at[share], loc_sem.at[1])
    prepare_values(0)
    if pair > 1:
        await_bytes(vraw.at[share], kv_recv.at[1])
        prepare_values(1)
        await_bytes(kbuf, kv_send.at[0])

    def body(p, carry):
        @pl.when(p < 2)
        def _():
            for d in range(1, chips):
                send_query(d, p).wait_recv()

        @pl.when((p >= 2) & (p % 2 == 0))
        def _():
            for d in range(1, chips):
                send_query(d, p, 2).wait_recv()

        for d in range(chips):
            buf = d % 2
            if not ping:
                find_scores(d, p, buf)
            elif d + 1 < chips:
                find_scores(d + 1, p, 1 - buf)
            else:
                find_scores(0, (p + 1) % steps, 1 - buf)
            if d == 0:
                finish_own(p, buf)
            else:
                finish_other(d, p, buf)
        return carry

    lax.fori_loop(0, steps, body, 0)

    pad[...] = jnp.zeros_like(pad)

    def await_group(send, d, p):
        @pl.when(p >= steps - 2)
        def _():
            send(d, p).wait_recv()

        @pl.when((p < steps - 2) & (p % 2 == 0))
        def _():
            send(d, p, 2).wait_recv()

    def combine(p, carry):
        mine = own_stat[p]
        top = mine
        got = []
        for d in range(1, chips):
            await_group(send_stats, d, p)
            pad[0 : STACK + 1] = stat_in[d, p]
            got.append(jnp.transpose(pad[...]))
            top = jnp.maximum(top, got[-1])
        mine = jnp.exp2(mine - top)
        factors = [jnp.exp2(both - top) for both in got]
        total = mine
        for factor in factors:
            total = total + factor
        inverse = 1.0 / total
        mine = mine * inverse
        factors = [factor * inverse for factor in factors]
        scales = [
            [factors[d - 1][:, u : u + 1] * got[d - 1][:, STACK : STACK + 1] for d in range(1, chips)]
            for u in range(STACK)
        ]
        results = [own[p, :, u * DH : (u + 1) * DH] * mine[:, u : u + 1] for u in range(STACK)]
        for d in range(1, chips):
            await_group(send_codes, d, p)
            for u in range(STACK):
                codes = code_in[d, p, :, u * DH : (u + 1) * DH].astype(jnp.int32).astype(jnp.float32)
                results[u] = results[u] + codes * scales[u][d - 1]
        results = [result.astype(jnp.bfloat16) for result in results]
        out_ref[:, columns(p)] = jnp.concatenate(results, axis=1)
        return carry

    lax.fori_loop(0, steps, combine, 0)

    for d in range(1, chips):
        send_query(d, 0, steps).wait_send()
        send_codes(d, 0, steps).wait_send()
        send_stats(d, 0, steps).wait_send()


def on_device(queries, new_keys, new_values, cache_keys, cache_values, valid_len, block_of):
    n = lax.axis_size("seq")
    pair = 2 if n % 2 == 0 else 1
    chips = n // pair
    rows, cols = queries.shape
    kv_cols = new_keys.shape[1]
    length = cache_keys.shape[0]
    steps = cols // (STACK * DH)
    links = max(1, chips - 1)
    pinned = [
        pltpu.with_memory_space_constraint(x, pltpu.HBM)
        for x in (
            queries, new_keys, new_values, cache_keys, cache_values, valid_len, block_of,
        )
    ]
    everywhere = pl.BlockSpec(memory_space=pl.ANY)
    dma = pltpu.SemaphoreType.DMA
    keys = pair * (length + rows)
    return pl.pallas_call(
        functools.partial(kernel, n, pair),
        out_shape=pltpu.VMEM((rows, cols), jnp.bfloat16),
        in_specs=[everywhere] * 7,
        out_specs=pl.BlockSpec(memory_space=pltpu.VMEM),
        scratch_shapes=[
            pltpu.VMEM((keys, kv_cols), jnp.bfloat16),
            pltpu.VMEM((keys, kv_cols), jnp.bfloat16),
            pltpu.VMEM((keys, 2 * kv_cols), jnp.bfloat16),
            pltpu.VMEM((chips, steps, rows, STACK * DH), jnp.bfloat16),
            pltpu.VMEM((STACK * rows, keys), jnp.float32),
            pltpu.VMEM((STACK * rows, keys), jnp.float32),
            pltpu.VMEM((STACK * rows, DH), jnp.float32),
            pltpu.VMEM((STACK * rows, DH), jnp.float32),
            pltpu.VMEM((steps, rows, STACK * DH), jnp.float32),
            pltpu.VMEM((steps, rows, DH), jnp.float32),
            pltpu.VMEM((chips, steps, rows, STACK * DH), jnp.int16),
            pltpu.VMEM((chips, steps, rows, STACK * DH), jnp.int16),
            pltpu.VMEM((chips, steps, STACK + 1, rows), jnp.float32),
            pltpu.VMEM((chips, steps, STACK + 1, rows), jnp.float32),
            pltpu.VMEM((chips, rows, pair * rows), jnp.float32),
            pltpu.VMEM((pair, 8, DH), jnp.float32),
            pltpu.VMEM((rows, DH), jnp.float32),
            pltpu.SMEM(valid_len.shape, jnp.int32),
            pltpu.SMEM(block_of.shape, jnp.int32),
            dma((4,)), dma((2,)), dma((1,)), dma((2,)),
            dma((links,)), dma((links, steps // 2 + 1)),
            dma((links,)), dma((links, steps // 2 + 1)),
            dma((links,)), dma((links, steps // 2 + 1)),
        ],
        compiler_params=pltpu.CompilerParams(
            collective_id=0, has_side_effects=True, vmem_limit_bytes=48 * 1024 * 1024,
        ),
    )(*pinned)


def solution(mesh):
    placed = (
        P(("groups", "seq"), "head"),
        P(("groups", "seq"), "head"),
        P(("groups", "seq"), "head"),
        P(("groups", "seq"), "head"),
        P(("groups", "seq"), "head"),
        P("groups"),
        P("groups"),
    )
    return jax.shard_map(
        on_device,
        mesh=mesh,
        in_specs=placed,
        out_specs=P(("groups", "seq"), "head"),
        check_vma=False,
    )
```

```python
import functools
import math

import jax
import jax.numpy as jnp
from jax import lax
from jax.experimental import pallas as pl
from jax.experimental.pallas import tpu as pltpu
from jax.sharding import PartitionSpec as P

DH = 128
GROUP = 8
NEGATIVE = -1e30
TO_LOG2 = DH ** (-0.5) * math.log2(math.e)
CODE_MAX = 32767.0
STACK = 2
TILE = 256


def kernel(
    n, pair,
    q_hbm, nk_hbm, nv_hbm, ck_hbm, cv_hbm, valid_hbm, block_hbm,
    out_ref,
    kbuf, vraw, vbuf, qbuf, score_a, score_b, top_a, top_b, own, own_stat,
    code_out, code_in, stat_out, stat_in, span_bias, repeat, pad, valid_ref, block_ref,
    loc_sem, ql_sem, kv_send, kv_recv, q_send, q_recv, r_send, r_recv, s_send, s_recv,
):
    chips = n // pair
    rows, cols = q_hbm.shape
    length, kv_cols = ck_hbm.shape
    kv_heads = kv_cols // DH
    heads = cols // DH
    steps = heads // STACK
    width = STACK * DH
    cached = pair * length
    keys = cached + pair * rows
    tiles = [(t, min(TILE, cached - t)) for t in range(0, cached, TILE)]
    tiles += [(cached + t, min(TILE, keys - cached - t)) for t in range(0, keys - cached, TILE)]
    me = lax.axis_index("seq")
    chip, core = me // pair, me % pair
    partner = chip * pair + (pair - 1 - core)

    def ahead(d):
        return ((chip + d) % chips) * pair + (pair - 1 - core)

    def behind(d):
        return ((chip + chips - d) % chips) * pair + (pair - 1 - core)

    barrier = pltpu.get_barrier_semaphore()
    others = [ahead(d) for d in range(1, chips)] + ([partner] if pair > 1 else [])
    for other in others:
        pl.semaphore_signal(barrier, inc=1, device_id={"seq": other})

    def columns(p):
        return pl.ds(pl.multiple_of(p * width, width), width)

    def local_query(p):
        return pltpu.make_async_copy(q_hbm.at[:, columns(p)], qbuf.at[0, p], ql_sem.at[min(p, 1)])

    def await_bytes(ref, sem):
        pltpu.make_async_copy(ref, ref, sem).wait()

    sources = (ck_hbm, nk_hbm, cv_hbm, nv_hbm)

    def place(i, slot):
        buf = kbuf if i < 2 else vraw
        start, size = ((slot * length, length), (cached + slot * rows, rows))[i % 2]
        return buf.at[pl.ds(start, size), :]

    local = [
        pltpu.make_async_copy(sources[i], place(i, 0), loc_sem.at[0]) for i in range(4)
    ] + [
        pltpu.make_async_copy(valid_hbm, valid_ref, loc_sem.at[1]),
        pltpu.make_async_copy(block_hbm, block_ref, loc_sem.at[2]),
    ]
    for p in range(steps):
        local_query(p).start()
    for copy in local:
        copy.start()

    pl.semaphore_wait(barrier, len(others))

    def send_query(d, p, count=1):
        return pltpu.make_async_remote_copy(
            src_ref=qbuf.at[0, pl.ds(p, count)], dst_ref=qbuf.at[d, pl.ds(p, count)],
            send_sem=q_send.at[d - 1], recv_sem=q_recv.at[d - 1, p // 2 + 1 if count == 2 else p],
            device_id={"seq": ahead(d)},
        )

    def code_slot(p, count):
        return {1: p - (steps - 2) // 2, 2: p // 2}.get(count, 0)

    def send_codes(d, p, count=1):
        return pltpu.make_async_remote_copy(
            src_ref=code_out.at[d, pl.ds(p, count)], dst_ref=code_in.at[d, pl.ds(p, count)],
            send_sem=r_send.at[d - 1], recv_sem=r_recv.at[d - 1, code_slot(p, count)],
            device_id={"seq": behind(d)},
        )

    def send_stats(d, p, count=1):
        return pltpu.make_async_remote_copy(
            src_ref=stat_out.at[d, pl.ds(p, count)], dst_ref=stat_in.at[d, pl.ds(p, count)],
            send_sem=s_send.at[d - 1], recv_sem=s_recv.at[d - 1, p - (steps - 3) if count == 1 else 0],
            device_id={"seq": behind(d)},
        )

    kv_copies = []
    if pair > 1:
        kv_copies = [
            pltpu.make_async_remote_copy(
                src_ref=sources[i], dst_ref=place(i, 1),
                send_sem=kv_send.at[0], recv_sem=kv_recv.at[0],
                device_id={"seq": partner},
            )
            for i in range(4)
        ]
    local_query(0).wait()
    for d in range(1, chips):
        send_query(d, 0).start()
    for copy in kv_copies:
        copy.start()
    await_bytes(qbuf.at[0, pl.ds(1, steps - 1)], ql_sem.at[1])
    for first, count in [(1, 1)] + [(p, 2) for p in range(2, steps, 2)]:
        for d in range(1, chips):
            send_query(d, first, count).start()

    local[4].wait()
    local[5].wait()
    key_owner = [me, partner][:pair]
    row_at = lax.broadcasted_iota(jnp.int32, (rows, rows), 0)
    col_at = lax.broadcasted_iota(jnp.int32, (rows, rows), 1)
    for d in range(chips):
        row_pos = block_ref[behind(d) if d else me] * rows + row_at
        for slot in range(pair):
            seen = block_ref[key_owner[slot]] * rows + col_at <= row_pos
            span_bias[d, :, slot * rows : (slot + 1) * rows] = jnp.where(seen, 0.0, NEGATIVE)

    lane = lax.broadcasted_iota(jnp.int32, (rows, DH), 1)
    slot_at = lax.broadcasted_iota(jnp.int32, (TILE, DH), 0)
    ones = jnp.ones((TILE, DH), jnp.bfloat16)

    def live_rows(slot, t):
        live = slot_at + t < valid_ref[key_owner[slot]]
        return jnp.where(live, 1.0, 0.0).astype(jnp.bfloat16)

    def prepare_keys(slot):
        first = kbuf[slot * length : slot * length + 1, :]
        for t in range(0, length, TILE):
            at = pl.ds(slot * length + t, TILE)
            live = live_rows(slot, t)
            for h in range(kv_heads):
                part = pl.ds(h * DH, DH)
                kbuf[at, part] = kbuf[at, part] * live + first[:, h * DH : (h + 1) * DH] * (ones - live)

    def prepare_values(slot):
        for t in range(0, length, TILE):
            at = pl.ds(slot * length + t, TILE)
            live = live_rows(slot, t)
            for h in range(kv_heads):
                vbuf[at, 2 * h * DH : (2 * h + 1) * DH] = vraw[at, h * DH : (h + 1) * DH] * live
                vbuf[at, (2 * h + 1) * DH : (2 * h + 2) * DH] = live
        at = pl.ds(cached + slot * rows, rows)
        for h in range(kv_heads):
            vbuf[at, 2 * h * DH : (2 * h + 1) * DH] = vraw[at, h * DH : (h + 1) * DH]
            vbuf[at, (2 * h + 1) * DH : (2 * h + 2) * DH] = jnp.ones((rows, DH), jnp.bfloat16)

    for slot in range(pair):
        copies = (length - valid_ref[key_owner[slot]]).astype(jnp.float32)
        repeat[slot] = jnp.where(lane[0:8] == 0, 1.0 - copies, 1.0)

    score = (score_a, score_b)
    peak = (top_a, top_b)

    def find_scores(d, p, buf):
        query = qbuf[d, p]
        stacked = jnp.concatenate([query[:, u * DH : (u + 1) * DH] for u in range(STACK)], axis=0)
        kv_at = pl.ds(pl.multiple_of(p * STACK // GROUP * DH, DH), DH)
        best = None
        for start, size in tiles:
            part = lax.dot_general(
                stacked, kbuf[start : start + size, kv_at], (((1,), (1,)), ((), ())),
                preferred_element_type=jnp.float32,
            )
            if start >= cached:
                bias = span_bias[d, :, start - cached : start - cached + size]
                part = part + jnp.concatenate([bias] * STACK, axis=0)
            score[buf][:, start : start + size] = part
            for c in range(0, size, DH):
                piece = part[:, c : c + DH]
                best = piece if best is None else jnp.maximum(best, piece)
        peak[buf][...] = jnp.broadcast_to(jnp.max(best, axis=1, keepdims=True), peak[buf].shape)

    def attend(p, buf):
        kv_at = pl.ds(pl.multiple_of(p * STACK // GROUP * (2 * DH), 2 * DH), 2 * DH)
        top = peak[buf][...]
        value = total = None
        for start, size in tiles:
            rounded = []
            for c in range(start, start + size, DH):
                weights = jnp.exp2((score[buf][:, c : c + DH] - top) * TO_LOG2)
                rounded.append(weights.astype(jnp.bfloat16))
                if c < cached and c % length == 0:
                    weights = weights * repeat[c // length, 0:1]
                total = weights if total is None else total + weights
            part = jnp.dot(
                jnp.concatenate(rounded, axis=1), vbuf[start : start + size, kv_at],
                preferred_element_type=jnp.float32,
            )
            value = part if value is None else value + part
        total = jnp.sum(total, axis=1, keepdims=True)
        return value[:, :DH] * (1.0 / total), top * TO_LOG2 + jnp.log2(total)

    def half(x, u):
        return x[u * rows : (u + 1) * rows]

    def finish_own(p, buf):
        value, level = attend(p, buf)
        own[p] = jnp.concatenate([half(value, u) for u in range(STACK)], axis=1)
        levels = half(level, 0)
        for u in range(1, STACK):
            levels = jnp.where(lane == u, half(level, u), levels)
        own_stat[p] = levels

    def finish_other(d, p, buf):
        value, level = attend(p, buf)
        size = jnp.abs(half(value, 0))
        for u in range(1, STACK):
            size = jnp.maximum(size, jnp.abs(half(value, u)))
        size = jnp.maximum(jnp.max(size, axis=1, keepdims=True), 1e-30)
        scale = CODE_MAX / size
        codes = [
            jnp.round(half(value, u) * scale).astype(jnp.int32).astype(jnp.int16)
            for u in range(STACK)
        ]
        code_out[d, p] = jnp.concatenate(codes, axis=1)
        stats = size * (1.0 / CODE_MAX)
        for u in range(STACK):
            stats = jnp.where(lane == u, half(level, u), stats)
        stat_out[d, p] = jnp.transpose(stats)[0 : STACK + 1]

        @pl.when(p >= steps - 2)
        def _():
            send_stats(d, p).start()
            send_codes(d, p).start()

        @pl.when((p < steps - 2) & (p % 2 == 1))
        def _():
            @pl.when(p == steps - 3)
            def _():
                send_stats(d, 0, steps - 2).start()

            send_codes(d, p - 1, 2).start()

    ping = chips % 2 == 0

    await_bytes(kbuf if pair > 1 else vbuf, loc_sem.at[0])
    prepare_keys(0)
    if pair > 1:
        await_bytes(kbuf, kv_recv.at[0])
        prepare_keys(1)
    if ping:
        find_scores(0, 0, 0)
    for slot in range(pair):
        prepare_values(slot)

    def body(p, carry):
        @pl.when(p < 2)
        def _():
            for d in range(1, chips):
                send_query(d, p).wait_recv()

        @pl.when((p >= 2) & (p % 2 == 0))
        def _():
            for d in range(1, chips):
                send_query(d, p, 2).wait_recv()

        for d in range(chips):
            buf = d % 2
            if not ping:
                find_scores(d, p, buf)
            elif d + 1 < chips:
                find_scores(d + 1, p, 1 - buf)
            else:
                find_scores(0, (p + 1) % steps, 1 - buf)
            if d == 0:
                finish_own(p, buf)
            else:
                finish_other(d, p, buf)
        return carry

    lax.fori_loop(0, steps, body, 0)

    pad[...] = jnp.zeros_like(pad)

    def await_codes(d, p):
        @pl.when(p >= steps - 2)
        def _():
            send_codes(d, p).wait_recv()

        @pl.when((p < steps - 2) & (p % 2 == 0))
        def _():
            send_codes(d, p, 2).wait_recv()

    def combine(p, carry):
        mine = own_stat[p]
        top = mine
        got = []
        for d in range(1, chips):
            @pl.when(p >= steps - 2)
            def _():
                send_stats(d, p).wait_recv()

            @pl.when(p == 0)
            def _():
                send_stats(d, 0, steps - 2).wait_recv()

            pad[0 : STACK + 1] = stat_in[d, p]
            got.append(jnp.transpose(pad[...]))
            top = jnp.maximum(top, got[-1])
        mine = jnp.exp2(mine - top)
        factors = [jnp.exp2(both - top) for both in got]
        total = mine
        for factor in factors:
            total = total + factor
        inverse = 1.0 / total
        mine = mine * inverse
        factors = [factor * inverse for factor in factors]
        scales = [
            [factors[d - 1][:, u : u + 1] * got[d - 1][:, STACK : STACK + 1] for d in range(1, chips)]
            for u in range(STACK)
        ]
        results = [own[p, :, u * DH : (u + 1) * DH] * mine[:, u : u + 1] for u in range(STACK)]
        for d in range(1, chips):
            await_codes(d, p)
            for u in range(STACK):
                codes = code_in[d, p, :, u * DH : (u + 1) * DH].astype(jnp.int32).astype(jnp.float32)
                results[u] = results[u] + codes * scales[u][d - 1]
        results = [result.astype(jnp.bfloat16) for result in results]
        out_ref[:, columns(p)] = jnp.concatenate(results, axis=1)
        return carry

    lax.fori_loop(0, steps, combine, 0)

    if pair > 1:
        await_bytes(kbuf, kv_send.at[0])
    for d in range(1, chips):
        send_query(d, 0, steps).wait_send()
        send_codes(d, 0, steps).wait_send()
        send_stats(d, 0, steps).wait_send()


def on_device(queries, new_keys, new_values, cache_keys, cache_values, valid_len, block_of):
    n = lax.axis_size("seq")
    pair = 2 if n % 2 == 0 else 1
    chips = n // pair
    rows, cols = queries.shape
    kv_cols = new_keys.shape[1]
    length = cache_keys.shape[0]
    steps = cols // (STACK * DH)
    links = max(1, chips - 1)
    pinned = [
        pltpu.with_memory_space_constraint(x, pltpu.HBM)
        for x in (
            queries, new_keys, new_values, cache_keys, cache_values, valid_len, block_of,
        )
    ]
    everywhere = pl.BlockSpec(memory_space=pl.ANY)
    dma = pltpu.SemaphoreType.DMA
    keys = pair * (length + rows)
    return pl.pallas_call(
        functools.partial(kernel, n, pair),
        out_shape=pltpu.VMEM((rows, cols), jnp.bfloat16),
        in_specs=[everywhere] * 7,
        out_specs=pl.BlockSpec(memory_space=pltpu.VMEM),
        scratch_shapes=[
            pltpu.VMEM((keys, kv_cols), jnp.bfloat16),
            pltpu.VMEM((keys, kv_cols), jnp.bfloat16),
            pltpu.VMEM((keys, 2 * kv_cols), jnp.bfloat16),
            pltpu.VMEM((chips, steps, rows, STACK * DH), jnp.bfloat16),
            pltpu.VMEM((STACK * rows, keys), jnp.float32),
            pltpu.VMEM((STACK * rows, keys), jnp.float32),
            pltpu.VMEM((STACK * rows, DH), jnp.float32),
            pltpu.VMEM((STACK * rows, DH), jnp.float32),
            pltpu.VMEM((steps, rows, STACK * DH), jnp.float32),
            pltpu.VMEM((steps, rows, DH), jnp.float32),
            pltpu.VMEM((chips, steps, rows, STACK * DH), jnp.int16),
            pltpu.VMEM((chips, steps, rows, STACK * DH), jnp.int16),
            pltpu.VMEM((chips, steps, STACK + 1, rows), jnp.float32),
            pltpu.VMEM((chips, steps, STACK + 1, rows), jnp.float32),
            pltpu.VMEM((chips, rows, pair * rows), jnp.float32),
            pltpu.VMEM((pair, 8, DH), jnp.float32),
            pltpu.VMEM((rows, DH), jnp.float32),
            pltpu.SMEM(valid_len.shape, jnp.int32),
            pltpu.SMEM(block_of.shape, jnp.int32),
            dma((3,)), dma((2,)), dma((1,)), dma((1,)),
            dma((links,)), dma((links, steps // 2 + 1)),
            dma((links,)), dma((links, steps // 2 + 1)),
            dma((links,)), dma((links, 3)),
        ],
        compiler_params=pltpu.CompilerParams(
            collective_id=0, has_side_effects=True, vmem_limit_bytes=48 * 1024 * 1024,
        ),
    )(*pinned)


def solution(mesh):
    placed = (
        P(("groups", "seq"), "head"),
        P(("groups", "seq"), "head"),
        P(("groups", "seq"), "head"),
        P(("groups", "seq"), "head"),
        P(("groups", "seq"), "head"),
        P("groups"),
        P("groups"),
    )
    return jax.shard_map(
        on_device,
        mesh=mesh,
        in_specs=placed,
        out_specs=P(("groups", "seq"), "head"),
        check_vma=False,
    )
```

```python
import functools
import math

import jax
import jax.numpy as jnp
from jax import lax
from jax.experimental import pallas as pl
from jax.experimental.pallas import tpu as pltpu
from jax.sharding import PartitionSpec as P

DH = 128
GROUP = 8
NEGATIVE = -1e30
TO_LOG2 = DH ** (-0.5) * math.log2(math.e)
CODE_MAX = 32767.0
STACK = 2
TILE = 256


def kernel(
    n, pair,
    q_hbm, nk_hbm, nv_hbm, ck_hbm, cv_hbm, valid_hbm, block_hbm,
    out_ref,
    kbuf, vraw, vbuf, qbuf, score_a, score_b, top_a, top_b, own, own_stat,
    code_out, code_in, stat_out, stat_in, span_bias, repeat, pad, valid_ref, block_ref,
    loc_sem, ql_sem, kv_send, kv_recv, q_send, q_recv, r_send, r_recv, s_send, s_recv,
):
    chips = n // pair
    rows, cols = q_hbm.shape
    length, kv_cols = ck_hbm.shape
    kv_heads = kv_cols // DH
    heads = cols // DH
    steps = heads // STACK
    width = STACK * DH
    cached = pair * length
    keys = cached + pair * rows
    tiles = [(t, min(TILE, cached - t)) for t in range(0, cached, TILE)]
    tiles += [(cached + t, min(TILE, keys - cached - t)) for t in range(0, keys - cached, TILE)]
    me = lax.axis_index("seq")
    chip, core = me // pair, me % pair
    partner = chip * pair + (pair - 1 - core)

    def ahead(d):
        return ((chip + d) % chips) * pair + (pair - 1 - core)

    def behind(d):
        return ((chip + chips - d) % chips) * pair + (pair - 1 - core)

    barrier = pltpu.get_barrier_semaphore()
    others = [ahead(d) for d in range(1, chips)] + ([partner] if pair > 1 else [])
    for other in others:
        pl.semaphore_signal(barrier, inc=1, device_id={"seq": other})

    def columns(p):
        return pl.ds(pl.multiple_of(p * width, width), width)

    def local_query(p):
        return pltpu.make_async_copy(q_hbm.at[:, columns(p)], qbuf.at[0, p], ql_sem.at[min(p, 1)])

    def await_bytes(ref, sem):
        pltpu.make_async_copy(ref, ref, sem).wait()

    sources = (ck_hbm, nk_hbm, cv_hbm, nv_hbm)

    def place(i, slot):
        buf = kbuf if i < 2 else vraw
        start, size = ((slot * length, length), (cached + slot * rows, rows))[i % 2]
        return buf.at[pl.ds(start, size), :]

    local = [
        pltpu.make_async_copy(sources[i], place(i, 0), loc_sem.at[i // 2]) for i in range(4)
    ] + [
        pltpu.make_async_copy(valid_hbm, valid_ref, loc_sem.at[2]),
        pltpu.make_async_copy(block_hbm, block_ref, loc_sem.at[3]),
    ]
    for p in range(steps):
        local_query(p).start()
    local[4].start()
    local[5].start()

    pl.semaphore_wait(barrier, len(others))

    def send_query(d, p, count=1):
        return pltpu.make_async_remote_copy(
            src_ref=qbuf.at[0, pl.ds(p, count)], dst_ref=qbuf.at[d, pl.ds(p, count)],
            send_sem=q_send.at[d - 1], recv_sem=q_recv.at[d - 1, p // 2 + 1 if count == 2 else p],
            device_id={"seq": ahead(d)},
        )

    def code_slot(p, count):
        return {1: p - (steps - 2) // 2, 2: p // 2}.get(count, 0)

    def send_codes(d, p, count=1):
        return pltpu.make_async_remote_copy(
            src_ref=code_out.at[d, pl.ds(p, count)], dst_ref=code_in.at[d, pl.ds(p, count)],
            send_sem=r_send.at[d - 1], recv_sem=r_recv.at[d - 1, code_slot(p, count)],
            device_id={"seq": behind(d)},
        )

    def send_stats(d, p, count=1):
        return pltpu.make_async_remote_copy(
            src_ref=stat_out.at[d, pl.ds(p, count)], dst_ref=stat_in.at[d, pl.ds(p, count)],
            send_sem=s_send.at[d - 1], recv_sem=s_recv.at[d - 1, code_slot(p, count)],
            device_id={"seq": behind(d)},
        )

    kv_copies = []
    if pair > 1:
        kv_copies = [
            pltpu.make_async_remote_copy(
                src_ref=sources[i], dst_ref=place(i, 1),
                send_sem=kv_send.at[0], recv_sem=kv_recv.at[i // 2],
                device_id={"seq": partner},
            )
            for i in range(4)
        ]
    local_query(0).wait()
    for d in range(1, chips):
        send_query(d, 0).start()
    for copy in kv_copies:
        copy.start()
    for copy in local[:4]:
        copy.start()
    await_bytes(qbuf.at[0, pl.ds(1, steps - 1)], ql_sem.at[1])
    for first, count in [(1, 1)] + [(p, 2) for p in range(2, steps, 2)]:
        for d in range(1, chips):
            send_query(d, first, count).start()

    local[4].wait()
    local[5].wait()
    key_owner = [me, partner][:pair]
    row_at = lax.broadcasted_iota(jnp.int32, (rows, rows), 0)
    col_at = lax.broadcasted_iota(jnp.int32, (rows, rows), 1)
    for d in range(chips):
        row_pos = block_ref[behind(d) if d else me] * rows + row_at
        for slot in range(pair):
            seen = block_ref[key_owner[slot]] * rows + col_at <= row_pos
            span_bias[d, :, slot * rows : (slot + 1) * rows] = jnp.where(seen, 0.0, NEGATIVE)

    lane = lax.broadcasted_iota(jnp.int32, (rows, DH), 1)
    slot_at = lax.broadcasted_iota(jnp.int32, (TILE, DH), 0)
    ones = jnp.ones((TILE, DH), jnp.bfloat16)

    def live_rows(slot, t):
        live = slot_at + t < valid_ref[key_owner[slot]]
        return jnp.where(live, 1.0, 0.0).astype(jnp.bfloat16)

    def prepare_keys(slot):
        first = kbuf[slot * length : slot * length + 1, :]
        for t in range(0, length, TILE):
            at = pl.ds(slot * length + t, TILE)
            live = live_rows(slot, t)
            for h in range(kv_heads):
                part = pl.ds(h * DH, DH)
                kbuf[at, part] = kbuf[at, part] * live + first[:, h * DH : (h + 1) * DH] * (ones - live)

    def prepare_values(slot):
        for t in range(0, length, TILE):
            at = pl.ds(slot * length + t, TILE)
            live = live_rows(slot, t)
            for h in range(kv_heads):
                vbuf[at, 2 * h * DH : (2 * h + 1) * DH] = vraw[at, h * DH : (h + 1) * DH] * live
                vbuf[at, (2 * h + 1) * DH : (2 * h + 2) * DH] = live
        at = pl.ds(cached + slot * rows, rows)
        for h in range(kv_heads):
            vbuf[at, 2 * h * DH : (2 * h + 1) * DH] = vraw[at, h * DH : (h + 1) * DH]
            vbuf[at, (2 * h + 1) * DH : (2 * h + 2) * DH] = jnp.ones((rows, DH), jnp.bfloat16)

    for slot in range(pair):
        copies = (length - valid_ref[key_owner[slot]]).astype(jnp.float32)
        repeat[slot] = jnp.where(lane[0:8] == 0, 1.0 - copies, 1.0)

    score = (score_a, score_b)
    peak = (top_a, top_b)

    def find_scores(d, p, buf):
        query = qbuf[d, p]
        stacked = jnp.concatenate([query[:, u * DH : (u + 1) * DH] for u in range(STACK)], axis=0)
        kv_at = pl.ds(pl.multiple_of(p * STACK // GROUP * DH, DH), DH)
        best = None
        for start, size in tiles:
            part = lax.dot_general(
                stacked, kbuf[start : start + size, kv_at], (((1,), (1,)), ((), ())),
                preferred_element_type=jnp.float32,
            )
            if start >= cached:
                bias = span_bias[d, :, start - cached : start - cached + size]
                part = part + jnp.concatenate([bias] * STACK, axis=0)
            score[buf][:, start : start + size] = part
            for c in range(0, size, DH):
                piece = part[:, c : c + DH]
                best = piece if best is None else jnp.maximum(best, piece)
        peak[buf][...] = jnp.broadcast_to(jnp.max(best, axis=1, keepdims=True), peak[buf].shape)

    def attend(p, buf):
        kv_at = pl.ds(pl.multiple_of(p * STACK // GROUP * (2 * DH), 2 * DH), 2 * DH)
        top = peak[buf][...]
        value = total = None
        for start, size in tiles:
            rounded = []
            for c in range(start, start + size, DH):
                weights = jnp.exp2((score[buf][:, c : c + DH] - top) * TO_LOG2)
                rounded.append(weights.astype(jnp.bfloat16))
                if c < cached and c % length == 0:
                    weights = weights * repeat[c // length, 0:1]
                total = weights if total is None else total + weights
            part = jnp.dot(
                jnp.concatenate(rounded, axis=1), vbuf[start : start + size, kv_at],
                preferred_element_type=jnp.float32,
            )
            value = part if value is None else value + part
        total = jnp.sum(total, axis=1, keepdims=True)
        return value[:, :DH] * (1.0 / total), top * TO_LOG2 + jnp.log2(total)

    def half(x, u):
        return x[u * rows : (u + 1) * rows]

    def finish_own(p, buf):
        value, level = attend(p, buf)
        own[p] = jnp.concatenate([half(value, u) for u in range(STACK)], axis=1)
        levels = half(level, 0)
        for u in range(1, STACK):
            levels = jnp.where(lane == u, half(level, u), levels)
        own_stat[p] = levels

    def finish_other(d, p, buf):
        value, level = attend(p, buf)
        size = jnp.abs(half(value, 0))
        for u in range(1, STACK):
            size = jnp.maximum(size, jnp.abs(half(value, u)))
        size = jnp.maximum(jnp.max(size, axis=1, keepdims=True), 1e-30)
        scale = CODE_MAX / size
        codes = [
            jnp.round(half(value, u) * scale).astype(jnp.int32).astype(jnp.int16)
            for u in range(STACK)
        ]
        code_out[d, p] = jnp.concatenate(codes, axis=1)
        stats = size * (1.0 / CODE_MAX)
        for u in range(STACK):
            stats = jnp.where(lane == u, half(level, u), stats)
        stat_out[d, p] = jnp.transpose(stats)[0 : STACK + 1]

        @pl.when(p >= steps - 2)
        def _():
            send_stats(d, p).start()
            send_codes(d, p).start()

        @pl.when((p < steps - 2) & (p % 2 == 1))
        def _():
            send_stats(d, p - 1, 2).start()
            send_codes(d, p - 1, 2).start()

    ping = chips % 2 == 0

    share = pl.ds(0, length + rows)
    await_bytes(kbuf.at[share], loc_sem.at[0])
    prepare_keys(0)
    if pair > 1:
        await_bytes(kbuf.at[share], kv_recv.at[0])
        prepare_keys(1)
    if ping:
        find_scores(0, 0, 0)
    await_bytes(vraw.at[share], loc_sem.at[1])
    prepare_values(0)
    if pair > 1:
        await_bytes(vraw.at[share], kv_recv.at[1])
        prepare_values(1)
        await_bytes(kbuf, kv_send.at[0])

    def body(p, carry):
        @pl.when(p < 2)
        def _():
            for d in range(1, chips):
                send_query(d, p).wait_recv()

        @pl.when((p >= 2) & (p % 2 == 0))
        def _():
            for d in range(1, chips):
                send_query(d, p, 2).wait_recv()

        for d in range(chips):
            buf = d % 2
            if not ping:
                find_scores(d, p, buf)
            elif d + 1 < chips:
                find_scores(d + 1, p, 1 - buf)
            else:
                find_scores(0, (p + 1) % steps, 1 - buf)
            if d == 0:
                finish_own(p, buf)
            else:
                finish_other(d, p, buf)
        return carry

    lax.fori_loop(0, steps, body, 0)

    pad[...] = jnp.zeros_like(pad)

    def await_group(send, d, p):
        @pl.when(p >= steps - 2)
        def _():
            send(d, p).wait_recv()

        @pl.when((p < steps - 2) & (p % 2 == 0))
        def _():
            send(d, p, 2).wait_recv()

    def combine(p, carry):
        mine = own_stat[p]
        top = mine
        got = []
        for d in range(1, chips):
            await_group(send_stats, d, p)
            pad[0 : STACK + 1] = stat_in[d, p]
            got.append(jnp.transpose(pad[...]))
            top = jnp.maximum(top, got[-1])
        mine = jnp.exp2(mine - top)
        factors = [jnp.exp2(both - top) for both in got]
        total = mine
        for factor in factors:
            total = total + factor
        inverse = 1.0 / total
        mine = mine * inverse
        factors = [factor * inverse for factor in factors]
        scales = [
            [factors[d - 1][:, u : u + 1] * got[d - 1][:, STACK : STACK + 1] for d in range(1, chips)]
            for u in range(STACK)
        ]
        results = [own[p, :, u * DH : (u + 1) * DH] * mine[:, u : u + 1] for u in range(STACK)]
        for d in range(1, chips):
            await_group(send_codes, d, p)
            for u in range(STACK):
                codes = code_in[d, p, :, u * DH : (u + 1) * DH].astype(jnp.int32).astype(jnp.float32)
                results[u] = results[u] + codes * scales[u][d - 1]
        results = [result.astype(jnp.bfloat16) for result in results]
        out_ref[:, columns(p)] = jnp.concatenate(results, axis=1)
        return carry

    lax.fori_loop(0, steps, combine, 0)

    for d in range(1, chips):
        send_query(d, 0, steps).wait_send()
        send_codes(d, 0, steps).wait_send()
        send_stats(d, 0, steps).wait_send()


def on_device(queries, new_keys, new_values, cache_keys, cache_values, valid_len, block_of):
    n = lax.axis_size("seq")
    pair = 2 if n % 2 == 0 else 1
    chips = n // pair
    rows, cols = queries.shape
    kv_cols = new_keys.shape[1]
    length = cache_keys.shape[0]
    steps = cols // (STACK * DH)
    links = max(1, chips - 1)
    pinned = [
        pltpu.with_memory_space_constraint(x, pltpu.HBM)
        for x in (
            queries, new_keys, new_values, cache_keys, cache_values, valid_len, block_of,
        )
    ]
    everywhere = pl.BlockSpec(memory_space=pl.ANY)
    dma = pltpu.SemaphoreType.DMA
    keys = pair * (length + rows)
    return pl.pallas_call(
        functools.partial(kernel, n, pair),
        out_shape=pltpu.VMEM((rows, cols), jnp.bfloat16),
        in_specs=[everywhere] * 7,
        out_specs=pl.BlockSpec(memory_space=pltpu.VMEM),
        scratch_shapes=[
            pltpu.VMEM((keys, kv_cols), jnp.bfloat16),
            pltpu.VMEM((keys, kv_cols), jnp.bfloat16),
            pltpu.VMEM((keys, 2 * kv_cols), jnp.bfloat16),
            pltpu.VMEM((chips, steps, rows, STACK * DH), jnp.bfloat16),
            pltpu.VMEM((STACK * rows, keys), jnp.float32),
            pltpu.VMEM((STACK * rows, keys), jnp.float32),
            pltpu.VMEM((STACK * rows, DH), jnp.float32),
            pltpu.VMEM((STACK * rows, DH), jnp.float32),
            pltpu.VMEM((steps, rows, STACK * DH), jnp.float32),
            pltpu.VMEM((steps, rows, DH), jnp.float32),
            pltpu.VMEM((chips, steps, rows, STACK * DH), jnp.int16),
            pltpu.VMEM((chips, steps, rows, STACK * DH), jnp.int16),
            pltpu.VMEM((chips, steps, STACK + 1, rows), jnp.float32),
            pltpu.VMEM((chips, steps, STACK + 1, rows), jnp.float32),
            pltpu.VMEM((chips, rows, pair * rows), jnp.float32),
            pltpu.VMEM((pair, 8, DH), jnp.float32),
            pltpu.VMEM((rows, DH), jnp.float32),
            pltpu.SMEM(valid_len.shape, jnp.int32),
            pltpu.SMEM(block_of.shape, jnp.int32),
            dma((4,)), dma((2,)), dma((1,)), dma((2,)),
            dma((links,)), dma((links, steps // 2 + 1)),
            dma((links,)), dma((links, steps // 2 + 1)),
            dma((links,)), dma((links, steps // 2 + 1)),
        ],
        compiler_params=pltpu.CompilerParams(
            collective_id=0, has_side_effects=True, vmem_limit_bytes=48 * 1024 * 1024,
        ),
    )(*pinned)


def solution(mesh):
    placed = (
        P(("groups", "seq"), "head"),
        P(("groups", "seq"), "head"),
        P(("groups", "seq"), "head"),
        P(("groups", "seq"), "head"),
        P(("groups", "seq"), "head"),
        P("groups"),
        P("groups"),
    )
    return jax.shard_map(
        on_device,
        mesh=mesh,
        in_specs=placed,
        out_specs=P(("groups", "seq"), "head"),
        check_vma=False,
    )
```
